128 devices in a mesh: gx: 16 (over y, x), gy: 8 (over z, core).
Axes of the slice: x: 4, y: 4, z: 4, core: 2. Of those that a mesh axis runs over, the one named last changes fastest.
Arguments:
- queries: bfloat16 [2048, 2048], P(('gx', 'gy')), may hold values from -6 to 6
- probe_dev: int32 [2048, 16], P(('gx', 'gy')), may hold values from 0 to 127, all different within a row; in each aligned block of 16 rows (0 to 15, 16 to 31, ...) at most 2 rows name the same one
- probe_list: int32 [2048, 16], P(('gx', 'gy')), may hold values from 0 to 15
- documents: bfloat16 [2048, 256, 2048], P(('gx', 'gy')), may hold values from -6 to 6
- lengths: int32 [2048], P(('gx', 'gy')), may hold values from 96 to 256, as said below
- short_dev: int32 [2048, 32], P(('gx', 'gy')), may hold values from 0 to 127, all different within a row; in each aligned block of 16 rows (0 to 15, 16 to 31, ...) at most 5 rows name the same one
- short_list: int32 [2048, 32], P(('gx', 'gy')), may hold values from 0 to 15
- short_row: int32 [2048, 32], P(('gx', 'gy')), may hold values from 0 to 95
Outputs:
- prefix_top: float32 [2048, 32], P(('gx', 'gy'))
- rescored: float32 [2048, 32], P(('gx', 'gy'))
The draws below stay inside these ranges and needn't reach their ends.
Inputs may be any that keep to these rules, and one draw needn't show every extreme that they name: `lengths`: every list holds at least 96 documents, and in every draw some list is full. `probe_dev`: the 16 entries of a query name different devices. Among the 16 queries of one device, no device is named more than 2 times, and some device is named exactly 2 times. `short_dev`: the 32 entries of a query name different devices. Among the 16 queries of one device, no device is named more than 5 times, and some device is named exactly 5 times.
All inputs are finite; a program needn't handle non-finite values.
Results may differ from the reference program's by a relative error of at most 0.0029.
Values may be sent and summed in bfloat16 or wider, within the bound.
A program may use at most 128 MiB of HBM per device.

```python
import math
import jax
import jax.numpy as jnp
import numpy as np
from jax import lax

QRY_DEV = 16
LISTS_DEV = 16
ROWS = 256
LEN_MIN = 96
PREFIX = 256
FULL = 2048
PROBES = 16
TOPK = 32
SHORT = 32
QUERIES = 2048
LISTS = 2048
CAP = 5
PCAP = 2
DEVICES = 128


def draw_lengths(key, part):
    first_key, second_key = jax.random.split(jax.random.fold_in(key, 17))
    counts = jax.random.randint(first_key, (LISTS,), LEN_MIN, ROWS + 1)
    full_spot = jax.random.randint(second_key, (), 0, LISTS)
    return jnp.where(jnp.arange(LISTS) == full_spot, ROWS, counts).astype(jnp.int32)


def plant(entries, key, smallest, top_value):
    spot = [jax.random.randint(jax.random.fold_in(key, axis), (), 0, length) for axis, length in enumerate(entries.shape)]
    main_axis = entries.shape.index(max(entries.shape))
    neighbour = spot[:main_axis] + [(spot[main_axis] + 1) % entries.shape[main_axis]] + spot[main_axis + 1:]
    return entries.at[tuple(spot)].set(smallest).at[tuple(neighbour)].set(top_value)


def steps_of(rng, extent, cuts, least, largest):
    factor_of, own = 1.0, jax.random.fold_in(rng, 6)
    for position, blocks in cuts:
        steps = jnp.exp(jax.random.uniform(jax.random.fold_in(own, position), (blocks,), jnp.float32, least / len(cuts), largest / len(cuts)))
        factor_of = factor_of * jnp.repeat(steps, extent[position] // blocks).reshape([-1 if axis == position else 1 for axis in range(len(extent))])
    return factor_of


def deal_out(own_key, own, number, rows, number_of, top, reach, skew):
    ranking = jax.random.permutation(own_key, number_of)
    heavy_load, ordinary = load_shares(number_of, rows * top, reach, skew, True), load_shares(number_of, rows * top, reach, skew, False)
    places = jnp.arange(number_of)

    def named(sizes, offset_by):
        used = int((sizes > 0).sum())
        fixed = max(1, used // 4)
        shifted = fixed + (places - fixed + offset_by * (used - fixed)) % max(1, number_of - fixed)
        return jnp.zeros((number_of,), jnp.int32).at[ranking[jnp.where(places < fixed, places, shifted)]].set(jnp.asarray(sizes, jnp.int32))

    sizes = jnp.where(number % 4 == 0, named(heavy_load, number // 4), named(ordinary, number - number // 4 - 1))
    mixed = jax.random.permutation(jax.random.fold_in(own, 3), number_of)
    giver, taker = mixed[0:number_of // 2 * 2:2], mixed[1:number_of // 2 * 2:2]
    margin = jnp.minimum(sizes[giver] - 1, reach - sizes[taker]) // 2
    margin = jnp.where((giver == ranking[0]) | (taker == ranking[0]) | (sizes[taker] == 0), 0, jnp.maximum(margin, 0))
    shifted = jax.random.randint(jax.random.fold_in(own, 4), (number_of // 2,), 0, 1 << 20) % (margin + 1)
    sizes = sizes.at[giver].add(-shifted).at[taker].add(shifted)
    members = jnp.searchsorted(jnp.cumsum(sizes), jnp.arange(rows * top), side="right").astype(jnp.int32)
    table = members.reshape(top, rows).T
    table = table[jax.random.permutation(jax.random.fold_in(own, 1), rows)]
    offset_by = jax.random.randint(jax.random.fold_in(own, 2), (rows, 1), 0, top)
    return jnp.take_along_axis(table, (jnp.arange(top)[None, :] + offset_by) % top, axis=1)


def load_shares(count, total, reach, skew, full):
    portions = [(1 << 20) // math.isqrt(grade ** skew) + 1 for grade in range(1, count + 1)]
    largest = reach if full else min(reach, max(-(-total // count), total * portions[0] // sum(portions)))
    least = 1 if total - largest >= count - 1 else 0
    given, rest = [largest] + [least] * (count - 1), total - largest - least * (count - 1)
    while rest > 0:
        movable = [i for i in range(1, count) if given[i] < largest] or [i for i in range(1, count) if given[i] < reach]
        whole, budget = sum([portions[i] for i in movable]), rest
        for i in movable:
            extra = min(reach - given[i], max(1, budget * portions[i] // whole), rest)
            given[i] = given[i] + extra
            rest = rest - extra
    return np.array(given)


def gaussian(rng, shape, deviation, bound, cuts=(), held_as=jnp.bfloat16):
    result = jax.random.normal(rng, shape, jnp.float32) * deviation
    if len(cuts) > 0:
        result = steps_of(rng, shape, cuts, -0.22, 0.18) * result
    return jnp.clip(result, min=-bound, max=bound).astype(held_as)


def setup_inputs(seed: int = 0) -> dict:
    key_of = jax.random.split(jax.random.key(seed), 9)
    queries = gaussian(key_of[0], (QUERIES, FULL), 1.0, 6.0, ((0, 128),))
    probe_dev_keys = jax.random.split(jax.random.fold_in(key_of[1], 1), QUERIES // QRY_DEV)
    probe_dev_turns = jax.random.permutation(jax.random.fold_in(key_of[1], 3), QUERIES // QRY_DEV)
    probe_dev = jax.vmap(lambda own, number: deal_out(jax.random.fold_in(key_of[1], 2), own, number, QRY_DEV, DEVICES, PROBES, PCAP, 2))(probe_dev_keys, probe_dev_turns).reshape((QUERIES, PROBES))
    probe_list = plant(jax.random.randint(key_of[2], (QUERIES, PROBES), 0, LISTS_DEV), jax.random.fold_in(key_of[2], 1), 0, LISTS_DEV - 1).astype(jnp.int32)
    documents = gaussian(key_of[3], (LISTS, ROWS, FULL), 1.0, 6.0, ((0, 128),))
    lengths = draw_lengths(jax.random.fold_in(key_of[8], 71), 0)
    short_dev_keys = jax.random.split(jax.random.fold_in(key_of[5], 1), QUERIES // QRY_DEV)
    short_dev_turns = jax.random.permutation(jax.random.fold_in(key_of[5], 3), QUERIES // QRY_DEV)
    short_dev = jax.vmap(lambda own, number: deal_out(jax.random.fold_in(key_of[5], 2), own, number, QRY_DEV, DEVICES, SHORT, CAP, 1))(short_dev_keys, short_dev_turns).reshape((QUERIES, SHORT))
    short_list = plant(jax.random.randint(key_of[6], (QUERIES, SHORT), 0, LISTS_DEV), jax.random.fold_in(key_of[6], 1), 0, LISTS_DEV - 1).astype(jnp.int32)
    short_row = plant(jax.random.randint(key_of[7], (QUERIES, SHORT), 0, LEN_MIN), jax.random.fold_in(key_of[7], 1), 0, LEN_MIN - 1).astype(jnp.int32)
    return dict(queries=queries, probe_dev=probe_dev, probe_list=probe_list, documents=documents, lengths=lengths, short_dev=short_dev, short_list=short_list, short_row=short_row)


def unit_rows(values):
    return values / jnp.sqrt(1.0 + lax.optimization_barrier(jnp.sum(values * values, axis=1, keepdims=True)))

def top_values(values, count):
    return -jnp.sort(-values, axis=-1)[..., :count]

def reference(queries, probe_dev, probe_list, documents, lengths, short_dev, short_list, short_row):
    query_float = queries.astype(jnp.float32)
    prefix_unit = unit_rows(query_float[:, :PREFIX]).astype(jnp.bfloat16)
    full_unit = unit_rows(query_float).astype(jnp.bfloat16)
    doc_prefix = documents[:, :, :PREFIX]
    probes = (probe_dev * LISTS_DEV + probe_list).astype(jnp.int32)
    query_total = queries.shape[0]
    block_rows = 64 if query_total % 64 == 0 else query_total

    def top_block(inputs):
        prefix_block, probe_block = inputs
        gathered = doc_prefix[probe_block]
        scores = jnp.einsum('bd,bprd->bpr', prefix_block.astype(jnp.float32), gathered.astype(jnp.float32))
        valid_rows = jnp.arange(ROWS)[None, None, :] < lengths[probe_block][:, :, None]
        masked = jnp.where(valid_rows, scores, -jnp.inf).reshape(prefix_block.shape[0], -1)
        return top_values(masked, TOPK)
    prefix_top = lax.map(top_block, (prefix_unit.reshape(-1, block_rows, PREFIX), probes.reshape(-1, block_rows, PROBES))).reshape(query_total, TOPK)

    def rescore_block(inputs):
        unit_block, dev_block, list_block, row_block = inputs
        list_index = (dev_block * LISTS_DEV + list_block).astype(jnp.int32)
        vectors = documents[list_index, row_block.astype(jnp.int32)]
        return jnp.einsum('bsf,bf->bs', vectors.astype(jnp.float32), unit_block.astype(jnp.float32))
    rescored = lax.map(rescore_block, (full_unit.reshape(-1, block_rows, FULL), short_dev.reshape(-1, block_rows, SHORT), short_list.reshape(-1, block_rows, SHORT), short_row.reshape(-1, block_rows, SHORT))).reshape(query_total, SHORT)
    return (prefix_top, rescored)
```

```python
import jax
import jax.numpy as jnp
from jax import lax
from jax.experimental import pallas as pl
from jax.experimental.pallas import tpu as pltpu
from jax.sharding import PartitionSpec as P

MESH = pl.DeviceIdType.MESH
SIDE = 4
DEVS = 128
QROWS = 16
LISTS = 16
ROWS = 256
ELIG = 96
PREFIX = 256
FULL = 2048
TILES = FULL // 128
CAP = 5
PCAP = 2
TOPK = 32
SHORT = 32
PROBES = 16
LOW = -1e30
PARTS = ((0, 6), (6, 11), (11, 16))
F32 = jnp.float32
BF16 = jnp.bfloat16
I32 = jnp.int32
LANE_CODE, LANE_ROW, LANE_LIST, LANE_PROW = 0, 8, 16, 24


def iota(shape, axis):
    return lax.broadcasted_iota(I32, shape, axis)


def merge_down(seq):
    seq = list(seq)
    step = len(seq) // 2
    while step:
        for i in range(len(seq)):
            if not i & step:
                a, b = seq[i], seq[i + step]
                seq[i], seq[i + step] = jnp.maximum(a, b), jnp.minimum(a, b)
        step //= 2
    return seq


def sort_down(seq):
    if len(seq) == 1:
        return list(seq)
    half = len(seq) // 2
    return merge_down(sort_down(seq[:half]) + sort_down(seq[half:])[::-1])


def join_rolled(seq, shift, axis):
    count = len(seq)
    other = [pltpu.roll(v, shift, axis) for v in seq]
    return merge_down([jnp.maximum(seq[i], other[count - 1 - i]) for i in range(count)])


def coords():
    gx, gy = lax.axis_index("gx"), lax.axis_index("gy")
    return gx // SIDE, gx % SIDE, gy // 2, gy % 2


def device_of(y, x, z, c):
    return (y * SIDE + x, z * 2 + c)


def at_offset(me, off):
    y = (me[0] + off // 32) % SIDE
    x = (me[1] + off // 8 % SIDE) % SIDE
    z = (me[2] + off // 2 % SIDE) % SIDE
    c = (me[3] + off % 2) % 2
    return device_of(y, x, z, c), (y * SIDE + x) * 8 + z * 2 + c


def back_offset(off):
    y = (SIDE - off // 32) % SIDE
    x = (SIDE - off // 8 % SIDE) % SIDE
    z = (SIDE - off // 2 % SIDE) % SIDE
    return (y * SIDE + x) * 8 + z * 2 + off % 2


class Gather:
    def __init__(self, qbuf, send_sem, recv_sem, me):
        self.qbuf, self.send_sem, self.recv_sem, self.me = qbuf, send_sem, recv_sem, me
        self.count = 0
        self.copies = []

    def view(self, where, tiles, core=0):
        return self.qbuf.at[where[0], where[1], where[2], core, tiles]

    def start(self, src, dst, peer):
        number = self.count
        self.count += 1
        copy = pltpu.make_async_remote_copy(
            src_ref=src,
            dst_ref=dst,
            send_sem=self.send_sem.at[number],
            recv_sem=self.recv_sem.at[number],
            device_id=peer,
            device_id_type=MESH,
        )
        copy.start()
        self.copies.append(copy)
        return copy

    def peer(self, axis, step):
        place = list(self.me)
        place[axis] = (place[axis] + SIDE + step) % SIDE
        return device_of(*place)

    def partner(self):
        y, x, z, c = self.me
        return device_of(y, x, z, 1 - c)

    def set_axis(self, unit, axis, value):
        where = list(unit)
        where[axis] = value
        return where

    def ring_start(self, unit, axis, tiles):
        own = self.view(self.set_axis(unit, axis, 0), tiles)
        fwd = self.start(own, self.view(self.set_axis(unit, axis, 3), tiles), self.peer(axis, 1))
        bwd = self.start(own, self.view(self.set_axis(unit, axis, 1), tiles), self.peer(axis, -1))
        middle = (tiles.start + tiles.stop + axis % 2) // 2
        halves = (slice(tiles.start, middle), slice(middle, tiles.stop))
        return dict(unit=unit, axis=axis, tiles=tiles, fwd=fwd, bwd=bwd, halves=halves)

    def ring_low(self, ring):
        ring["fwd"].wait_recv()
        unit, axis, tiles = ring["unit"], ring["axis"], ring["halves"][0]
        ring["end_fwd"] = self.start(
            self.view(self.set_axis(unit, axis, 3), tiles),
            self.view(self.set_axis(unit, axis, 2), tiles),
            self.peer(axis, 1),
        )

    def ring_high(self, ring):
        ring["bwd"].wait_recv()
        unit, axis, tiles = ring["unit"], ring["axis"], ring["halves"][1]
        ring["end_bwd"] = self.start(
            self.view(self.set_axis(unit, axis, 1), tiles),
            self.view(self.set_axis(unit, axis, 2), tiles),
            self.peer(axis, -1),
        )

    def ring_end(self, ring):
        ring["end_fwd"].wait_recv()
        ring["end_bwd"].wait_recv()

    def across(self, where, tiles):
        return self.start(self.view(where, tiles, 0), self.view(where, tiles, 1), self.partner())

    def run(self):
        every = slice(0, SIDE)
        rest = slice(1, SIDE)
        parts = []
        for number, (low, high) in enumerate(PARTS):
            axes = (number, (number + 1) % 3, (number + 2) % 3)
            parts.append(dict(axes=axes, tiles=slice(low, high)))

        def unit(axes, a, b, c):
            where = [0, 0, 0]
            where[axes[0]], where[axes[1]], where[axes[2]] = a, b, c
            return where

        partner = [self.across([0, 0, 0], slice(0, TILES))]
        for part in parts:
            a, b, c = part["axes"]
            part["A"] = self.ring_start([0, 0, 0], a, part["tiles"])
        for part in parts:
            a, b, c = part["axes"]
            part["B0"] = self.ring_start([0, 0, 0], b, part["tiles"])
            part["C0"] = self.ring_start([0, 0, 0], c, part["tiles"])
        for part in parts:
            self.ring_low(part["A"])
            self.ring_high(part["A"])
        for part in parts:
            for name in ("B0", "C0"):
                self.ring_low(part[name])
                self.ring_high(part[name])
        for part in parts:
            axes, tiles = part["axes"], part["tiles"]
            self.ring_end(part["A"])
            part["B1"] = self.ring_start(unit(axes, rest, 0, 0), axes[1], tiles)
            part["C1"] = self.ring_start(unit(axes, rest, 0, 0), axes[2], tiles)
            partner.append(self.across(unit(axes, rest, 0, 0), tiles))
        for part in parts:
            axes, tiles = part["axes"], part["tiles"]
            self.ring_low(part["B1"])
            part["C2"] = self.ring_start(unit(axes, every, 3, 0), axes[2], tiles)
            partner.append(self.across(unit(axes, every, 3, 0), tiles))
            self.ring_high(part["B1"])
            part["C3"] = self.ring_start(unit(axes, every, 1, 0), axes[2], tiles)
            partner.append(self.across(unit(axes, every, 1, 0), tiles))
        for part in parts:
            self.ring_low(part["C1"])
            self.ring_high(part["C1"])
        for part in parts:
            axes, tiles = part["axes"], part["tiles"]
            self.ring_end(part["B0"])
            self.ring_end(part["B1"])
            part["C4"] = self.ring_start(unit(axes, every, 2, 0), axes[2], tiles)
            partner.append(self.across(unit(axes, every, 2, 0), tiles))
        for part in parts:
            axes, tiles = part["axes"], part["tiles"]
            self.ring_end(part["C0"])
            partner.append(self.across(unit(axes, 0, 0, rest), tiles))
            self.ring_end(part["C1"])
            partner.append(self.across(unit(axes, rest, 0, rest), tiles))
        for name, b in (("C2", 3), ("C3", 1), ("C4", 2)):
            for part in parts:
                axes, tiles = part["axes"], part["tiles"]
                self.ring_low(part[name])
                partner.append(self.across(unit(axes, every, b, 3), tiles))
                self.ring_high(part[name])
                partner.append(self.across(unit(axes, every, b, 1), tiles))
        for name, b in (("C2", 3), ("C3", 1), ("C4", 2)):
            for part in parts:
                axes, tiles = part["axes"], part["tiles"]
                self.ring_end(part[name])
                partner.append(self.across(unit(axes, every, b, 2), tiles))
        for copy in partner:
            copy.wait_recv()
        for copy in self.copies:
            copy.wait_send()


def kernel(
    q_hbm, docs_hbm, lengths, sdev_ref, slist_ref, srow_ref, pdev_ref, plist_ref,
    ptop_ref, resc_ref,
    qbuf, docs, dpre, gath, oh, psel, sel, tabsend, tabrecv, psend, precv, rsend, rrecv,
    load_sem, gsend, grecv, xsend, xrecv,
):
    me = coords()
    own_number = (me[0] * SIDE + me[1]) * 8 + me[2] * 2 + me[3]

    for t in range(TILES):
        pltpu.make_async_copy(
            q_hbm.at[:, pl.ds(t * 128, 128)], qbuf.at[0, 0, 0, 0, t], load_sem.at[0]
        ).start()
    docs_copy = pltpu.make_async_copy(docs_hbm.at[:, pl.ds(0, ELIG), :], docs, load_sem.at[1])
    docs_copy.start()
    dpre_copy = pltpu.make_async_copy(docs_hbm.at[:, :, pl.ds(0, PREFIX)], dpre, load_sem.at[2])
    dpre_copy.start()

    barrier = pltpu.get_barrier_semaphore()

    def greet(off, carry):
        peer, _ = at_offset(me, off)
        pl.semaphore_signal(barrier, inc=1, device_id=peer, device_id_type=MESH)
        return carry

    lax.fori_loop(1, DEVS, greet, 0)

    dev = iota((QROWS, DEVS), 1)
    sdev = sdev_ref[...]
    scode = (slist_ref[...] * ELIG + srow_ref[...] + 1).astype(F32)
    pdev = pdev_ref[...]
    pcode = (plist_ref[...] + 1).astype(F32)
    lower = (iota((QROWS, QROWS), 1) < iota((QROWS, QROWS), 0)).astype(F32).astype(BF16)
    qnum = iota((QROWS, DEVS), 0).astype(F32) + 1.0

    def table(devs, codes, width):
        got = jnp.zeros((QROWS, DEVS), F32)
        for s in range(width):
            got = got + jnp.where(devs[:, s : s + 1] == dev, codes[:, s : s + 1], 0.0)
        used = jnp.where(got > 0.0, 1.0, 0.0)
        rank = jnp.dot(lower, used.astype(BF16), preferred_element_type=F32)
        return got, jnp.where(used > 0.0, rank, -1.0)

    stab, srank = table(sdev, scode, SHORT)
    ptab, prank = table(pdev, pcode, PROBES)
    krow = iota((32, DEVS), 0)
    slots = jnp.zeros((32, DEVS), F32)
    for base, row_base, tab, rank, cap in (
        (LANE_CODE, LANE_ROW, stab, srank, CAP),
        (LANE_LIST, LANE_PROW, ptab, prank, PCAP),
    ):
        for j in range(cap):
            hit = rank == float(j)
            code = jnp.sum(jnp.where(hit, tab, 0.0), axis=0, keepdims=True) - 1.0
            row = jnp.sum(jnp.where(hit, qnum, 0.0), axis=0, keepdims=True) - 1.0
            slots = jnp.where(krow == base + j, code, slots)
            slots = jnp.where(krow == row_base + j, row, slots)
    slots = jnp.concatenate([slots, jnp.zeros((96, DEVS), F32)], axis=0)
    tabsend[...] = slots.T.astype(I32).reshape(DEVS, 1, DEVS)

    pltpu.make_async_copy(qbuf.at[0, 0, 0, 1], qbuf.at[0, 0, 0, 0], load_sem.at[0]).wait()
    pl.semaphore_wait(barrier, DEVS - 1)

    def exchange(send, recv, number, by_offset):
        def body(off, carry):
            peer, flat = at_offset(me, off)
            if by_offset:
                src, dst = send.at[off], recv.at[own_number]
            else:
                src, dst = send.at[flat], recv.at[back_offset(off)]
            pltpu.make_async_remote_copy(
                src_ref=src, dst_ref=dst, send_sem=xsend.at[number], recv_sem=xrecv.at[number],
                device_id=peer, device_id_type=MESH,
            ).start()
            return carry

        lax.fori_loop(1, DEVS, body, 0)

    def exchanged(send, recv, number):
        rest = pl.ds(0, DEVS - 1)
        pltpu.make_async_copy(recv.at[rest], recv.at[rest], xrecv.at[number]).wait()
        pltpu.make_async_copy(send.at[rest], send.at[rest], xsend.at[number]).wait()

    exchange(tabsend, tabrecv, 0, False)
    gather = Gather(qbuf, gsend, grecv, me)
    gather.run()
    exchanged(tabsend, tabrecv, 0)
    tabrecv[0] = tabsend[own_number]
    docs_copy.wait()
    dpre_copy.wait()

    slot = tabrecv[...].reshape(DEVS, DEVS)
    slot_t = slot.astype(F32).T

    doc_number = iota((DEVS, LISTS * ELIG), 1)
    for j in range(CAP):
        hit = slot[:, LANE_CODE + j : LANE_CODE + j + 1] == doc_number
        oh[pl.ds(j * DEVS, DEVS), :] = jnp.where(hit, 1.0, 0.0).astype(BF16)

    def pick(n, carry):
        cols = pl.ds(pl.multiple_of(n * 256, 256), 256)
        block = docs[:, :, cols].reshape(LISTS * ELIG, 256)
        got = jnp.dot(oh[...], block, preferred_element_type=F32)
        gath[:, :, cols] = got.astype(BF16).reshape(CAP, DEVS, 256)
        return carry

    lax.fori_loop(0, FULL // 256, pick, 0)

    def queries(g, t):
        half = g % 2
        return qbuf[g // 2, pl.ds(half * 2, 2), :, :, t].reshape(256, 128)

    group_row = iota((16, 1), 0)
    group_col = iota((16, 256), 1)

    def own_column(rows, lane):
        number = rows[:, lane : lane + 1]
        return jnp.where(number < 0, -1, group_row * QROWS + number)

    def prefixes(g, carry):
        here = pl.ds(pl.multiple_of(g * 16, 16), 16)
        rows = tabrecv[here].reshape(16, DEVS)
        hits = [
            jnp.where(own_column(rows, LANE_PROW + p) == group_col, 1.0, 0.0) for p in range(PCAP)
        ]
        hit = jnp.concatenate(hits, axis=0).astype(BF16)
        for t in range(PREFIX // 128):
            got = jnp.dot(hit, queries(g, t), preferred_element_type=F32).astype(BF16)
            psel[:, here, pl.ds(t * 128, 128)] = got.reshape(PCAP, 16, 128)
        return carry

    lax.fori_loop(0, 8, prefixes, 0)

    lists = jnp.concatenate([slot_t[LANE_LIST + p : LANE_LIST + p + 1, :] for p in range(PCAP)], axis=1)
    wanted = psel[...].reshape(PCAP * DEVS, PREFIX)
    rows_valid = jnp.zeros((1, PCAP * DEVS), I32)
    for n in range(LISTS):
        rows_valid = jnp.where(lists == float(n), lengths[n], rows_valid)

    def score(n, carry):
        got = lax.dot_general(
            dpre[n], wanted, (((1,), (1,)), ((), ())), preferred_element_type=F32
        )
        sel[...] = jnp.where(lists == n.astype(F32), got, sel[...])
        return carry

    sel[...] = jnp.zeros_like(sel)
    lax.fori_loop(0, LISTS, score, 0)

    sub = iota((8, DEVS), 0)
    tops = []
    for p in range(PCAP):
        lanes = pl.ds(p * DEVS, DEVS)
        bound = rows_valid[:, p * DEVS : (p + 1) * DEVS]
        seq = [
            jnp.where(sub + v * 8 < bound, sel[pl.ds(v * 8, 8), lanes], LOW) for v in range(32)
        ]
        seq = sort_down(seq)
        for shift in (4, 2, 1):
            seq = join_rolled(seq, shift, 0)
        for m in range(TOPK // 8):
            block = seq[m * 8]
            for s in range(1, 8):
                block = jnp.where(sub == s, seq[m * 8 + s], block)
            tops.append(block)
    tops.append(jnp.zeros((DEVS - PCAP * TOPK, DEVS), F32))
    psend[...] = jnp.concatenate(tops, axis=0).T.reshape(DEVS, 1, DEVS)
    exchange(psend, precv, 1, True)

    lane = iota((16, DEVS), 1)

    def rescore(g, carry):
        here = pl.ds(pl.multiple_of(g * 16, 16), 16)
        rows = tabrecv[here].reshape(16, DEVS)
        got = jnp.zeros((CAP * 16, 256), F32)
        for k in range(FULL // 256):
            left = gath[:, here, pl.ds(k * 256, 256)].reshape(CAP * 16, 256)
            right = jnp.concatenate([queries(g, 2 * k), queries(g, 2 * k + 1)], axis=1)
            got = got + lax.dot_general(
                left, right, (((1,), (1,)), ((), ())), preferred_element_type=F32
            )
        out = jnp.zeros((16, DEVS), F32)
        for j in range(CAP):
            hit = own_column(rows, LANE_ROW + j) == group_col
            value = jnp.sum(
                jnp.where(hit, got[j * 16 : (j + 1) * 16, :], 0.0), axis=1, keepdims=True
            )
            out = jnp.where(lane == j, value, out)
        rsend[here] = out.reshape(16, 1, DEVS)
        return carry

    lax.fori_loop(0, 8, rescore, 0)
    exchange(rsend, rrecv, 2, True)

    squares = jnp.zeros((QROWS, 128), F32)
    for t in range(TILES):
        value = qbuf[0, 0, 0, 0, t].astype(F32)
        squares = squares + value * value
        if t == PREFIX // 128 - 1:
            prefix_squares = squares
    full_scale = 1.0 / jnp.sqrt(1.0 + jnp.sum(squares, axis=1, keepdims=True))
    prefix_scale = 1.0 / jnp.sqrt(1.0 + jnp.sum(prefix_squares, axis=1, keepdims=True))

    exchanged(psend, precv, 1)
    precv[own_number] = psend[0]
    back = precv[...].reshape(DEVS, DEVS).T
    first, second = prank == 0.0, prank == 1.0
    seq = [
        jnp.where(first, back[k : k + 1, :], jnp.where(second, back[TOPK + k : TOPK + k + 1, :], LOW))
        for k in range(TOPK)
    ]
    for shift in (64, 32, 16, 8, 4, 2, 1):
        seq = join_rolled(seq, shift, 1)
    best = seq[0]
    for k in range(1, TOPK):
        best = jnp.where(lane == k, seq[k], best)
    ptop_ref[...] = (best * prefix_scale)[:, :TOPK]

    exchanged(rsend, rrecv, 2)
    rrecv[own_number] = rsend[0]
    back = rrecv[...].reshape(DEVS, DEVS).T
    value = jnp.zeros((QROWS, DEVS), F32)
    for j in range(CAP):
        value = jnp.where(srank == float(j), back[j : j + 1, :], value)
    out = jnp.zeros((QROWS, DEVS), F32)
    for s in range(SHORT):
        one = jnp.sum(
            jnp.where(sdev[:, s : s + 1] == dev, value, 0.0), axis=1, keepdims=True
        )
        out = jnp.where(lane == s, one, out)
    resc_ref[...] = (out * full_scale)[:, :SHORT]


COPIES = 3 * 32 + 1 + 3 * 15


def shards(queries, probe_dev, probe_list, documents, lengths, short_dev, short_list, short_row):
    vmem = pl.BlockSpec(memory_space=pltpu.VMEM)
    anywhere = pl.BlockSpec(memory_space=pl.ANY)
    row = (DEVS, 1, DEVS)
    return pl.pallas_call(
        kernel,
        name="search",
        out_shape=(
            jax.ShapeDtypeStruct((QROWS, TOPK), F32),
            jax.ShapeDtypeStruct((QROWS, SHORT), F32),
        ),
        in_specs=[anywhere, anywhere, pl.BlockSpec(memory_space=pltpu.SMEM)] + [vmem] * 5,
        out_specs=(vmem, vmem),
        scratch_shapes=[
            pltpu.VMEM((SIDE, SIDE, SIDE, 2, TILES, QROWS, 128), BF16),
            pltpu.VMEM((LISTS, ELIG, FULL), BF16),
            pltpu.VMEM((LISTS, ROWS, PREFIX), BF16),
            pltpu.VMEM((CAP, DEVS, FULL), BF16),
            pltpu.VMEM((CAP * DEVS, LISTS * ELIG), BF16),
            pltpu.VMEM((PCAP, DEVS, PREFIX), BF16),
            pltpu.VMEM((ROWS, PCAP * DEVS), F32),
            pltpu.VMEM(row, I32),
            pltpu.VMEM(row, I32),
            pltpu.VMEM(row, F32),
            pltpu.VMEM(row, F32),
            pltpu.VMEM(row, F32),
            pltpu.VMEM(row, F32),
            pltpu.SemaphoreType.DMA((3,)),
            pltpu.SemaphoreType.DMA((COPIES,)),
            pltpu.SemaphoreType.DMA((COPIES,)),
            pltpu.SemaphoreType.DMA((3,)),
            pltpu.SemaphoreType.DMA((3,)),
        ],
        compiler_params=pltpu.CompilerParams(
            collective_id=0, has_side_effects=True, vmem_limit_bytes=60 * 1024 * 1024
        ),
    )(queries, documents, lengths, short_dev, short_list, short_row, probe_dev, probe_list)


def solution(mesh):
    spread = P(("gx", "gy"), None)
    in_specs = (spread, spread, spread, P(("gx", "gy"), None, None), P(("gx", "gy")), spread, spread, spread)
    return jax.shard_map(shards, mesh=mesh, in_specs=in_specs, out_specs=(spread, spread), check_vma=False)
```

```python
import jax
import jax.numpy as jnp
from jax import lax
from jax.experimental import pallas as pl
from jax.experimental.pallas import tpu as pltpu
from jax.sharding import PartitionSpec as P

MESH = pl.DeviceIdType.MESH
SIDE = 4
DEVS = 128
QROWS = 16
LISTS = 16
ROWS = 256
ELIG = 96
PREFIX = 256
FULL = 2048
TILES = FULL // 128
CAP = 5
PCAP = 2
TOPK = 32
SHORT = 32
PROBES = 16
LOW = -1e30
PARTS = ((0, 6), (6, 12), (12, 16))
F32 = jnp.float32
BF16 = jnp.bfloat16
I32 = jnp.int32
LANE_CODE, LANE_ROW, LANE_LIST = 0, 5, 10
RINGS = 8


def iota(shape, axis):
    return lax.broadcasted_iota(I32, shape, axis)


def merge_down(seq):
    seq = list(seq)
    step = len(seq) // 2
    while step:
        for i in range(len(seq)):
            if not i & step:
                a, b = seq[i], seq[i + step]
                seq[i], seq[i + step] = jnp.maximum(a, b), jnp.minimum(a, b)
        step //= 2
    return seq


def sort_down(seq):
    if len(seq) == 1:
        return list(seq)
    half = len(seq) // 2
    return merge_down(sort_down(seq[:half]) + sort_down(seq[half:])[::-1])


def join_rolled(seq, shift, axis):
    count = len(seq)
    other = [pltpu.roll(v, shift, axis) for v in seq]
    return merge_down([jnp.maximum(seq[i], other[count - 1 - i]) for i in range(count)])


def coords():
    gx, gy = lax.axis_index("gx"), lax.axis_index("gy")
    return gx // SIDE, gx % SIDE, gy // 2, gy % 2


def device_of(y, x, z, c):
    return (y * SIDE + x, z * 2 + c)


def for_peers(me, visit):
    steps = range(SIDE)
    xs = [(me[1] + d) % SIDE for d in steps]
    zs = [(me[2] + d) % SIDE * 2 for d in steps]
    gys = [[z + me[3], z + 1 - me[3]] for z in zs]

    def visit_one(dy, back_dy, gx, dx, dz, dc):
        gy = gys[dz][dc]
        off = dy * 32 + (dx * 8 + dz * 2 + dc)
        back = back_dy * 32 + ((SIDE - dx) % SIDE * 8 + (SIDE - dz) % SIDE * 2 + dc)
        visit((gx, gy), gx * 8 + gy, off, back)

    def plane(dy, carry):
        back_dy = (SIDE - dy) % SIDE
        row = (me[0] + dy) % SIDE * SIDE
        for dx in steps:
            gx = row + xs[dx]
            for dz in steps:
                for dc in range(2):
                    if dx or dz or dc:
                        visit_one(dy, back_dy, gx, dx, dz, dc)
        return carry

    for dy in range(1, SIDE):
        visit_one(dy, SIDE - dy, (me[0] + dy) % SIDE * SIDE + xs[0], 0, 0, 0)
    lax.fori_loop(0, SIDE, plane, 0)


class Gather:
    def __init__(self, qbuf, send_sem, recv_sem, cross_sem, me):
        self.qbuf, self.send_sem, self.recv_sem = qbuf, send_sem, recv_sem
        self.cross_sem, self.me = cross_sem, me
        self.count = 0
        y, x, z, c = me
        self.partner = device_of(y, x, z, 1 - c)
        self.peers = {}
        for axis in range(3):
            for step in (1, 2, 3):
                place = list(me)
                place[axis] = (place[axis] + step) % SIDE
                self.peers[axis, step] = device_of(*place)

    def view(self, where, tiles, core=0):
        return self.qbuf.at[where[0], where[1], where[2], core, tiles]

    def next_sem(self):
        self.count += 1
        return self.recv_sem.at[self.count - 1]

    def start(self, src, dst, peer, sem):
        copy = pltpu.make_async_remote_copy(
            src_ref=src, dst_ref=dst, send_sem=self.send_sem, recv_sem=sem,
            device_id=peer, device_id_type=MESH,
        )
        copy.start()
        return copy

    def slot(self, ring, value, tiles):
        where = list(ring["unit"])
        where[ring["axis"]] = value
        return self.view(where, tiles)

    def ring_start(self, unit, axis, tiles, far=False):
        ring = dict(unit=unit, axis=axis, tiles=tiles, end=self.next_sem())
        own = self.slot(ring, 0, tiles)
        ring["fwd"] = self.start(own, self.slot(ring, 3, tiles), self.peers[axis, 1], self.next_sem())
        ring["bwd"] = self.start(own, self.slot(ring, 1, tiles), self.peers[axis, 3], self.next_sem())
        if far:
            self.start(own, self.slot(ring, 2, tiles), self.peers[axis, 2], ring["end"])
        return ring

    def ring_low(self, ring, relay=True):
        ring["fwd"].wait_recv()
        if relay:
            tiles = slice(ring["tiles"].start, (ring["tiles"].start + ring["tiles"].stop) // 2)
            src, dst = self.slot(ring, 3, tiles), self.slot(ring, 2, tiles)
            self.start(src, dst, self.peers[ring["axis"], 1], ring["end"])

    def ring_high(self, ring, relay=True):
        ring["bwd"].wait_recv()
        if relay:
            tiles = slice((ring["tiles"].start + ring["tiles"].stop) // 2, ring["tiles"].stop)
            src, dst = self.slot(ring, 1, tiles), self.slot(ring, 2, tiles)
            self.start(src, dst, self.peers[ring["axis"], 3], ring["end"])

    def ring_end(self, ring):
        far = self.slot(ring, 2, ring["tiles"])
        pltpu.make_async_copy(far, far, ring["end"]).wait()

    def across(self, where, tiles):
        self.start(self.view(where, tiles, 0), self.view(where, tiles, 1), self.partner, self.cross_sem)

    def begin(self):
        self.parts = []
        for number, (low, high) in enumerate(PARTS):
            axes = (number, (number + 1) % 3, (number + 2) % 3)
            self.parts.append(dict(axes=axes, tiles=slice(low, high)))
        home = [0, 0, 0]
        for part in self.parts:
            part["A"] = self.ring_start(home, part["axes"][0], part["tiles"], far=True)
        for part in self.parts:
            part["B0"] = self.ring_start(home, part["axes"][1], part["tiles"])
            part["C0"] = self.ring_start(home, part["axes"][2], part["tiles"])
        self.across(home, slice(0, TILES))

    def run(self, work):
        every = slice(0, SIDE)
        rest = slice(1, SIDE)
        parts = self.parts

        def unit(part, a, b, c):
            where = [0, 0, 0]
            for axis, value in zip(part["axes"], (a, b, c)):
                where[axis] = value
            return where

        def to_c(part, name, a, b):
            where = unit(part, a, b, 0)
            part[name] = self.ring_start(where, part["axes"][2], part["tiles"])
            self.across(where, part["tiles"])

        for part in parts:
            self.ring_low(part["A"], relay=False)
            self.ring_high(part["A"], relay=False)
        for part in parts:
            for name in ("B0", "C0"):
                self.ring_low(part[name])
                self.ring_high(part[name])
        for part in parts:
            self.ring_end(part["A"])
            part["B1"] = self.ring_start(unit(part, rest, 0, 0), part["axes"][1], part["tiles"])
            to_c(part, "C1", rest, 0)
        work(0)
        for part in parts:
            self.ring_low(part["B1"])
            self.ring_high(part["B1"])
            to_c(part, "C2", every, 3)
            to_c(part, "C3", every, 1)
        work(1)
        for part in parts:
            self.ring_low(part["C1"])
            self.ring_high(part["C1"])
        work(2)
        for part in parts:
            self.ring_end(part["B0"])
            self.ring_end(part["B1"])
            to_c(part, "C4", every, 2)
        work(3)
        for part in parts:
            self.ring_end(part["C0"])
            self.across(unit(part, 0, 0, rest), part["tiles"])
            self.ring_end(part["C1"])
            self.across(unit(part, rest, 0, rest), part["tiles"])
        work(4)
        for name, b in (("C2", 3), ("C3", 1)):
            for part in parts:
                self.ring_low(part[name])
                self.across(unit(part, every, b, 3), part["tiles"])
                self.ring_high(part[name])
                self.across(unit(part, every, b, 1), part["tiles"])
            work(5 if b == 3 else 6)
        for name, b in (("C4", 2),):
            for part in parts:
                self.ring_low(part[name])
                self.across(unit(part, every, b, 3), part["tiles"])
                self.ring_high(part[name])
                self.across(unit(part, every, b, 1), part["tiles"])
        work(7)
        for name, b in (("C2", 3), ("C3", 1), ("C4", 2)):
            for part in parts:
                self.ring_end(part[name])
                self.across(unit(part, every, b, 2), part["tiles"])
        work(8)
        half = self.qbuf.at[:, :, :, 1]
        pltpu.make_async_copy(half, half, self.cross_sem).wait()

    def drain(self):
        rest = slice(1, SIDE)
        for ref in (
            self.qbuf.at[rest], self.qbuf.at[0, rest], self.qbuf.at[0, 0, rest], self.qbuf.at[0, 0, 0, 1]
        ):
            pltpu.make_async_copy(ref, ref, self.send_sem).wait()


def kernel(
    q_hbm, docs_hbm, lengths, sdev_ref, slist_ref, srow_ref, pdev_ref, plist_ref,
    ptop_ref, resc_ref,
    qbuf, docs, dpre, gath, oh, sel, slot_ref, ask, asked, psend, precv, rsend, rrecv,
    load_sem, gsend, grecv, gcross, xsend, xrecv,
):
    me = coords()
    own_number = (me[0] * SIDE + me[1]) * 8 + me[2] * 2 + me[3]
    for t in range(TILES):
        pltpu.make_async_copy(
            q_hbm.at[:, pl.ds(t * 128, 128)], qbuf.at[0, 0, 0, 0, t], load_sem.at[0]
        ).start()
    barrier = pltpu.get_barrier_semaphore()

    def greet(peer, flat, off, back):
        pl.semaphore_signal(barrier, inc=1, device_id=peer, device_id_type=MESH)

    for_peers(me, greet)
    docs_copy = pltpu.make_async_copy(docs_hbm.at[:, pl.ds(0, ELIG), :], docs, load_sem.at[1])
    docs_copy.start()
    dpre_copy = pltpu.make_async_copy(docs_hbm.at[:, :, pl.ds(0, PREFIX)], dpre, load_sem.at[2])
    dpre_copy.start()

    dev = iota((QROWS, DEVS), 1)
    sdev = sdev_ref[...]
    scode = (slist_ref[...] * ELIG + srow_ref[...] + 1).astype(F32)
    pdev = pdev_ref[...]
    pcode = (plist_ref[...] + 1).astype(F32)
    lower = (iota((QROWS, QROWS), 1) < iota((QROWS, QROWS), 0)).astype(F32).astype(BF16)
    qnum = iota((QROWS, DEVS), 0).astype(F32) + 1.0

    def table(devs, codes, width):
        got = jnp.zeros((QROWS, DEVS), F32)
        for s in range(width):
            got = got + jnp.where(devs[:, s : s + 1] == dev, codes[:, s : s + 1], 0.0)
        used = jnp.where(got > 0.0, 1.0, 0.0)
        rank = jnp.dot(lower, used.astype(BF16), preferred_element_type=F32)
        return got, jnp.where(used > 0.0, rank, -1.0)

    stab, srank = table(sdev, scode, SHORT)
    ptab, prank = table(pdev, pcode, PROBES)
    krow = iota((16, DEVS), 0)
    slots = jnp.zeros((16, DEVS), F32)
    for base, row_base, tab, rank, cap in (
        (LANE_CODE, LANE_ROW, stab, srank, CAP),
        (LANE_LIST, None, ptab, prank, PCAP),
    ):
        for j in range(cap):
            hit = rank == float(j)
            code = jnp.sum(jnp.where(hit, tab, 0.0), axis=0, keepdims=True) - 1.0
            slots = jnp.where(krow == base + j, code, slots)
            if row_base is not None:
                row = jnp.sum(jnp.where(hit, qnum, 0.0), axis=0, keepdims=True) - 1.0
                slots = jnp.where(krow == row_base + j, row, slots)
    both = jnp.concatenate([slots, prank, jnp.zeros((96, DEVS), F32)], axis=0).T
    ask[:, :, pl.ds(PCAP * PREFIX, DEVS)] = both.reshape(DEVS, 1, DEVS)

    pltpu.make_async_copy(qbuf.at[0, 0, 0, 1], qbuf.at[0, 0, 0, 0], load_sem.at[0]).wait()
    squares = jnp.zeros((QROWS, 128), F32)
    for t in range(TILES):
        value = qbuf[0, 0, 0, 0, t].astype(F32)
        squares = squares + value * value
        if t == PREFIX // 128 - 1:
            prefix_squares = squares
    full_norm = jnp.sqrt(1.0 + jnp.sum(squares, axis=1, keepdims=True))
    prefix_norm = jnp.sqrt(1.0 + jnp.sum(prefix_squares, axis=1, keepdims=True))
    for p in range(PCAP):
        hit = jnp.where(both[:, 16:32] == float(p), 1.0, 0.0).astype(BF16)
        for t in range(PREFIX // 128):
            unit = (qbuf[0, 0, 0, 0, t].astype(F32) / prefix_norm).astype(BF16)
            rows = jnp.dot(hit, unit, preferred_element_type=F32)
            ask[:, :, pl.ds(p * PREFIX + t * 128, 128)] = rows.reshape(DEVS, 1, 128)

    pl.semaphore_wait(barrier, DEVS - 1)

    def exchange(send, recv, number, by_offset):
        def visit(peer, flat, off, back):
            if by_offset:
                src, dst = send.at[off], recv.at[own_number]
            else:
                src, dst = send.at[flat], recv.at[back]
            pltpu.make_async_remote_copy(
                src_ref=src, dst_ref=dst, send_sem=xsend.at[number], recv_sem=xrecv.at[number],
                device_id=peer, device_id_type=MESH,
            ).start()

        for_peers(me, visit)

    def exchanged(send, recv, number):
        rest = pl.ds(0, DEVS - 1)
        pltpu.make_async_copy(recv.at[rest], recv.at[rest], xrecv.at[number]).wait()
        pltpu.make_async_copy(send.at[rest], send.at[rest], xsend.at[number]).wait()

    gather = Gather(qbuf, gsend, grecv, gcross, me)
    gather.begin()
    exchange(ask, asked, 0, False)

    lane = iota((16, DEVS), 1)

    def read_slots():
        exchanged(ask, asked, 0)
        asked[0] = ask[own_number]
        docs_copy.wait()
        dpre_copy.wait()
        slot_ref[...] = asked[:, :, pl.ds(PCAP * PREFIX, DEVS)].reshape(DEVS, DEVS).astype(I32)

    def mark(j):
        doc_number = iota((DEVS, LISTS * ELIG), 1)
        hit = slot_ref[:, LANE_CODE + j : LANE_CODE + j + 1] == doc_number
        oh[pl.ds(j * DEVS, DEVS), :] = jnp.where(hit, 1.0, 0.0).astype(BF16)

    def pick(low, high):
        def body(n, carry):
            cols = pl.ds(pl.multiple_of(n * 256, 256), 256)
            block = docs[:, :, cols].reshape(LISTS * ELIG, 256)
            got = jnp.dot(oh[...], block, preferred_element_type=F32)
            gath[:, :, cols] = got.astype(BF16).reshape(CAP, DEVS, 256)
            return carry

        lax.fori_loop(low, high, body, 0)

    def prefix_scores():
        slot_t = slot_ref[...].astype(F32).T
        lists = jnp.concatenate(
            [slot_t[LANE_LIST + p : LANE_LIST + p + 1, :] for p in range(PCAP)], axis=1
        )
        wanted = jnp.concatenate(
            [asked[:, :, pl.ds(p * PREFIX, PREFIX)].reshape(DEVS, PREFIX) for p in range(PCAP)], axis=0
        ).T.astype(BF16)
        sel[...] = jnp.zeros_like(sel)
        for n in range(LISTS):
            got = jnp.dot(dpre[n], wanted, preferred_element_type=F32)
            sel[...] = jnp.where(lists == float(n), got, sel[...])
        rows_valid = jnp.zeros((1, PCAP * DEVS), I32)
        for n in range(LISTS):
            rows_valid = jnp.where(lists == float(n), lengths[n], rows_valid)
        sub = iota((8, DEVS), 0)
        tops = []
        for p in range(PCAP):
            lanes = pl.ds(p * DEVS, DEVS)
            bound = rows_valid[:, p * DEVS : (p + 1) * DEVS]
            seq = [
                jnp.where(sub + v * 8 < bound, sel[pl.ds(v * 8, 8), lanes], LOW) for v in range(32)
            ]
            seq = sort_down(seq)
            for shift in (4, 2, 1):
                seq = join_rolled(seq, shift, 0)
            for m in range(TOPK // 8):
                block = seq[m * 8]
                for s in range(1, 8):
                    block = jnp.where(sub == s, seq[m * 8 + s], block)
                tops.append(block)
        tops.append(jnp.zeros((DEVS - PCAP * TOPK, DEVS), F32))
        psend[...] = jnp.concatenate(tops, axis=0).T.reshape(DEVS, 1, DEVS)

    def return_prefix():
        exchange(psend, precv, 1, True)

    def merge_prefix():
        exchanged(psend, precv, 1)
        precv[own_number] = psend[0]
        back = precv[...].reshape(DEVS, DEVS).T
        first, second = prank == 0.0, prank == 1.0
        seq = [
            jnp.where(
                first, back[k : k + 1, :], jnp.where(second, back[TOPK + k : TOPK + k + 1, :], LOW)
            )
            for k in range(TOPK)
        ]
        for shift in (64, 32, 16, 8, 4, 2, 1):
            seq = join_rolled(seq, shift, 1)
        best = seq[0]
        for k in range(1, TOPK):
            best = jnp.where(lane == k, seq[k], best)
        ptop_ref[...] = best[:, :TOPK]

    def work(stage):
        if stage == 1:
            read_slots()
            for j in range(CAP):
                mark(j)
        elif stage == 2:
            prefix_scores()
            return_prefix()
        elif stage == 3:
            pick(0, 2)
        elif stage == 4:
            pick(2, 4)
        elif stage == 5:
            pick(4, 6)
        elif stage == 6:
            pick(6, 8)
        elif stage == 8:
            merge_prefix()

    gather.run(work)

    group_row = iota((16, 1), 0)
    group_col = iota((16, 256), 1)

    def queries(g, t):
        return qbuf[g // 2, pl.ds(g % 2 * 2, 2), :, :, t].reshape(256, 128)

    def rescore(g, carry):
        here = pl.ds(pl.multiple_of(g * 16, 16), 16)
        rows = slot_ref[here]
        got = jnp.zeros((CAP * 16, 256), F32)
        for k in range(FULL // 256):
            left = gath[:, here, pl.ds(k * 256, 256)].reshape(CAP * 16, 256)
            right = jnp.concatenate([queries(g, 2 * k), queries(g, 2 * k + 1)], axis=1)
            got = got + lax.dot_general(
                left, right, (((1,), (1,)), ((), ())), preferred_element_type=F32
            )
        out = jnp.zeros((16, DEVS), F32)
        for j in range(CAP):
            number = rows[:, LANE_ROW + j : LANE_ROW + j + 1]
            hit = jnp.where(number < 0, -1, group_row * QROWS + number) == group_col
            value = jnp.sum(
                jnp.where(hit, got[j * 16 : (j + 1) * 16, :], 0.0), axis=1, keepdims=True
            )
            out = jnp.where(lane == j, value, out)
        rsend[here] = out.reshape(16, 1, DEVS)
        return carry

    lax.fori_loop(0, 8, rescore, 0, unroll=2)
    exchange(rsend, rrecv, 2, True)
    gather.drain()
    exchanged(rsend, rrecv, 2)
    rrecv[own_number] = rsend[0]
    back = rrecv[...].reshape(DEVS, DEVS).T
    value = jnp.zeros((QROWS, DEVS), F32)
    for j in range(CAP):
        value = jnp.where(srank == float(j), back[j : j + 1, :], value)
    out = jnp.zeros((QROWS, DEVS), F32)
    for s in range(SHORT):
        one = jnp.sum(jnp.where(sdev[:, s : s + 1] == dev, value, 0.0), axis=1, keepdims=True)
        out = jnp.where(lane == s, one, out)
    resc_ref[...] = (out / full_norm)[:, :SHORT]


def shards(queries, probe_dev, probe_list, documents, lengths, short_dev, short_list, short_row):
    vmem = pl.BlockSpec(memory_space=pltpu.VMEM)
    anywhere = pl.BlockSpec(memory_space=pl.ANY)
    return pl.pallas_call(
        kernel,
        name="search",
        out_shape=(
            jax.ShapeDtypeStruct((QROWS, TOPK), F32),
            jax.ShapeDtypeStruct((QROWS, SHORT), F32),
        ),
        in_specs=[anywhere, anywhere, pl.BlockSpec(memory_space=pltpu.SMEM)] + [vmem] * 5,
        out_specs=(vmem, vmem),
        scratch_shapes=[
            pltpu.VMEM((SIDE, SIDE, SIDE, 2, TILES, QROWS, 128), BF16),
            pltpu.VMEM((LISTS, ELIG, FULL), BF16),
            pltpu.VMEM((LISTS, ROWS, PREFIX), BF16),
            pltpu.VMEM((CAP, DEVS, FULL), BF16),
            pltpu.VMEM((CAP * DEVS, LISTS * ELIG), BF16),
            pltpu.VMEM((ROWS, PCAP * DEVS), F32),
            pltpu.VMEM((DEVS, DEVS), I32),
            pltpu.VMEM((DEVS, 1, PCAP * PREFIX + DEVS), F32),
            pltpu.VMEM((DEVS, 1, PCAP * PREFIX + DEVS), F32),
            pltpu.VMEM((DEVS, 1, DEVS), F32),
            pltpu.VMEM((DEVS, 1, DEVS), F32),
            pltpu.VMEM((DEVS, 1, DEVS), F32),
            pltpu.VMEM((DEVS, 1, DEVS), F32),
            pltpu.SemaphoreType.DMA((3,)),
            pltpu.SemaphoreType.DMA,
            pltpu.SemaphoreType.DMA((RINGS * 9,)),
            pltpu.SemaphoreType.DMA,
            pltpu.SemaphoreType.DMA((3,)),
            pltpu.SemaphoreType.DMA((3,)),
        ],
        compiler_params=pltpu.CompilerParams(
            collective_id=0, has_side_effects=True, vmem_limit_bytes=60 * 1024 * 1024
        ),
    )(queries, documents, lengths, short_dev, short_list, short_row, probe_dev, probe_list)


def solution(mesh):
    spread = P(("gx", "gy"), None)
    in_specs = (spread, spread, spread, P(("gx", "gy"), None, None), P(("gx", "gy")), spread, spread, spread)
    return jax.shard_map(shards, mesh=mesh, in_specs=in_specs, out_specs=(spread, spread), check_vma=False)
```

```python
import jax
import jax.numpy as jnp
from jax import lax
from jax.experimental import pallas as pl
from jax.experimental.pallas import tpu as pltpu
from jax.sharding import PartitionSpec as P

MESH = pl.DeviceIdType.MESH
SIDE = 4
DEVS = 128
QROWS = 16
LISTS = 16
ROWS = 256
ELIG = 96
PREFIX = 256
FULL = 2048
TILES = FULL // 128
CAP = 5
PCAP = 2
TOPK = 32
SHORT = 32
PROBES = 16
LOW = -1e30
PARTS = ((0, 2, 2), (2, 7, 0), (7, 12, 1), (12, 16, 2))
F32 = jnp.float32
BF16 = jnp.bfloat16
I32 = jnp.int32
LANE_CODE, LANE_ROW, LANE_LIST, LANE_PROW = 0, 5, 10, 12
RINGS = 8


def iota(shape, axis):
    return lax.broadcasted_iota(I32, shape, axis)


def merge_down(seq):
    seq = list(seq)
    step = len(seq) // 2
    while step:
        for i in range(len(seq)):
            if not i & step:
                a, b = seq[i], seq[i + step]
                seq[i], seq[i + step] = jnp.maximum(a, b), jnp.minimum(a, b)
        step //= 2
    return seq


def sort_down(seq):
    if len(seq) == 1:
        return list(seq)
    half = len(seq) // 2
    return merge_down(sort_down(seq[:half]) + sort_down(seq[half:])[::-1])


def join_rolled(seq, shift, axis):
    count = len(seq)
    other = [pltpu.roll(v, shift, axis) for v in seq]
    return merge_down([jnp.maximum(seq[i], other[count - 1 - i]) for i in range(count)])


def coords():
    gx, gy = lax.axis_index("gx"), lax.axis_index("gy")
    return gx // SIDE, gx % SIDE, gy // 2, gy % 2


def device_of(y, x, z, c):
    return (y * SIDE + x, z * 2 + c)


FAR_FIRST = (2, 1, 3, 0)
EVERY, REST = slice(0, SIDE), slice(1, SIDE)
NEAR, FAR = (("C2", 3), ("C3", 1)), (("C4", 2),)


class Peers:
    def __init__(self, me):
        self.rows = [(me[0] + d) % SIDE * SIDE for d in range(SIDE)]
        self.xs = [(me[1] + d) % SIDE for d in range(SIDE)]
        zs = [(me[2] + d) % SIDE * 2 for d in range(SIDE)]
        self.gys = [[z + me[3], z + 1 - me[3]] for z in zs]
        self.me = me

    def each(self, visit):
        def visit_one(dy, back_dy, gx, dx, dz, dc):
            gy = self.gys[dz][dc]
            off = dy * 16 + (dc * 64 + dx * 4 + dz)
            back = back_dy * 16 + (dc * 64 + (SIDE - dx) % SIDE * 4 + (SIDE - dz) % SIDE)
            visit((gx, gy), gx * 8 + gy, off, back)

        def plane(number, carry):
            dy = (number + 2) % SIDE
            row = (self.me[0] + dy) % SIDE * SIDE
            for dx in FAR_FIRST:
                gx = row + self.xs[dx]
                for dz in FAR_FIRST:
                    for dc in range(2):
                        if dx or dz or dc:
                            visit_one(dy, (SIDE - dy) % SIDE, gx, dx, dz, dc)
            return carry

        lax.fori_loop(0, SIDE, plane, 0)
        for dy in range(1, SIDE):
            visit_one(dy, SIDE - dy, self.rows[dy] + self.xs[0], 0, 0, 0)

    def group(self, g):
        for dx in FAR_FIRST:
            for dz in FAR_FIRST:
                if g or dx or dz:
                    yield dx // 2, (self.rows[g % SIDE] + self.xs[dx], self.gys[dz][g // SIDE])


class Gather:
    def __init__(self, qbuf, send_sem, recv_sem, cross_sem, me):
        self.qbuf, self.send_sem, self.recv_sem = qbuf, send_sem, recv_sem
        self.cross_sem, self.me = cross_sem, me
        self.count = 0
        y, x, z, c = me
        self.partner = device_of(y, x, z, 1 - c)
        self.peers = {}
        for axis in range(3):
            for step in (1, 2, 3):
                place = list(me)
                place[axis] = (place[axis] + step) % SIDE
                self.peers[axis, step] = device_of(*place)

    def view(self, where, tiles, core=0):
        return self.qbuf.at[where[0], where[1], where[2], core, tiles]

    def next_sem(self):
        self.count += 1
        return self.recv_sem.at[self.count - 1]

    def start(self, src, dst, peer, sem):
        copy = pltpu.make_async_remote_copy(
            src_ref=src, dst_ref=dst, send_sem=self.send_sem, recv_sem=sem,
            device_id=peer, device_id_type=MESH,
        )
        copy.start()
        return copy

    def slot(self, ring, value, tiles):
        where = list(ring["unit"])
        where[ring["axis"]] = value
        return self.view(where, tiles)

    def ring_start(self, unit, axis, tiles, far=False):
        ring = dict(unit=unit, axis=axis, tiles=tiles, end=self.next_sem())
        own = self.slot(ring, 0, tiles)
        ring["fwd"] = self.start(own, self.slot(ring, 3, tiles), self.peers[axis, 1], self.next_sem())
        ring["bwd"] = self.start(own, self.slot(ring, 1, tiles), self.peers[axis, 3], self.next_sem())
        if far:
            self.start(own, self.slot(ring, 2, tiles), self.peers[axis, 2], ring["end"])
        return ring

    def ring_low(self, ring, relay=True):
        ring["fwd"].wait_recv()
        if relay:
            tiles = slice(ring["tiles"].start, (ring["tiles"].start + ring["tiles"].stop) // 2)
            src, dst = self.slot(ring, 3, tiles), self.slot(ring, 2, tiles)
            self.start(src, dst, self.peers[ring["axis"], 1], ring["end"])

    def ring_high(self, ring, relay=True):
        ring["bwd"].wait_recv()
        if relay:
            tiles = slice((ring["tiles"].start + ring["tiles"].stop) // 2, ring["tiles"].stop)
            src, dst = self.slot(ring, 1, tiles), self.slot(ring, 2, tiles)
            self.start(src, dst, self.peers[ring["axis"], 3], ring["end"])

    def ring_end(self, ring):
        far = self.slot(ring, 2, ring["tiles"])
        pltpu.make_async_copy(far, far, ring["end"]).wait()

    def across(self, part, where):
        tiles = part["tiles"]
        self.start(
            self.view(where, tiles, 0), self.view(where, tiles, 1), self.partner, self.cross_sem.at[part["late"]]
        )

    def unit(self, part, a, b, c):
        where = [0, 0, 0]
        for axis, value in zip(part["axes"], (a, b, c)):
            where[axis] = value
        return where

    def to_c(self, part, name, a, b):
        where = self.unit(part, a, b, 0)
        part[name] = self.ring_start(where, part["axes"][2], part["tiles"])
        self.across(part, where)

    def begin(self):
        self.parts = []
        for low, high, first in PARTS:
            axes = (first, (first + 1) % 3, (first + 2) % 3)
            self.parts.append(dict(axes=axes, tiles=slice(low, high), late=int(low > 0)))
        home = [0, 0, 0]
        for part in self.parts:
            part["A"] = self.ring_start(home, part["axes"][0], part["tiles"], far=True)
        for name, order in (("B0", 1), ("C0", 2)):
            for part in self.parts:
                part[name] = self.ring_start(home, part["axes"][order], part["tiles"])
        for part in self.parts:
            self.across(part, home)

    def first_axis(self, parts):
        for part in parts:
            self.ring_low(part["A"], relay=False)
            self.ring_high(part["A"], relay=False)
            self.ring_end(part["A"])
            part["B1"] = self.ring_start(self.unit(part, REST, 0, 0), part["axes"][1], part["tiles"])

    def home_blocks(self, parts):
        for name in ("B0", "C0"):
            for part in parts:
                self.ring_low(part[name])
                self.ring_high(part[name])
        for part in parts:
            self.to_c(part, "C1", REST, 0)

    def second_axis(self, parts):
        for part in parts:
            self.ring_low(part["B1"])
            self.ring_high(part["B1"])
        for part in parts:
            self.to_c(part, "C2", EVERY, 3)
            self.to_c(part, "C3", EVERY, 1)

    def second_axis_end(self, parts):
        for part in parts:
            self.ring_end(part["B0"])
            self.ring_end(part["B1"])
            self.to_c(part, "C4", EVERY, 2)

    def third_axis_line(self, parts):
        for part in parts:
            self.ring_low(part["C1"])
            self.ring_high(part["C1"])

    def third_axis(self, parts, pairs):
        for name, b in pairs:
            for part in parts:
                self.ring_low(part[name])
                self.ring_high(part[name])
                self.across(part, self.unit(part, EVERY, b, 3))
                self.across(part, self.unit(part, EVERY, b, 1))

    def third_axis_line_end(self, parts):
        for part in parts:
            self.ring_end(part["C0"])
            self.across(part, self.unit(part, 0, 0, REST))
            self.ring_end(part["C1"])
            self.across(part, self.unit(part, REST, 0, REST))

    def third_axis_end(self, parts, pairs):
        for name, b in pairs:
            for part in parts:
                self.ring_end(part[name])
                self.across(part, self.unit(part, EVERY, b, 2))

    def wait_partner(self, late):
        low = PARTS[0][1]
        tiles = slice(low, TILES) if late else slice(0, low)
        half = self.qbuf.at[:, :, :, 1, tiles]
        pltpu.make_async_copy(half, half, self.cross_sem.at[late]).wait()

    def drain(self):
        rest = slice(1, SIDE)
        for ref in (
            self.qbuf.at[rest], self.qbuf.at[0, rest], self.qbuf.at[0, 0, rest], self.qbuf.at[0, 0, 0, 1]
        ):
            pltpu.make_async_copy(ref, ref, self.send_sem).wait()


def kernel(
    q_hbm, docs_hbm, lengths_hbm, sdev_hbm, slist_hbm, srow_hbm, pdev_hbm, plist_hbm,
    out_ref,
    lengths, sdev_ref, slist_ref, srow_ref, pdev_ref, plist_ref,
    qbuf, docs, dpre, gath, oh, sel, slot_ref, psel, ask, asked, psend, precv, rsend, rrecv,
    small_sem, load_sem, gsend, grecv, gcross, xsend, xrecv,
):
    me = coords()
    own_number = (me[0] * SIDE + me[1]) * 8 + me[2] * 2 + me[3]
    peers = Peers(me)
    barrier = pltpu.get_barrier_semaphore()
    small = [
        pltpu.make_async_copy(src, dst, small_sem.at[n])
        for n, (src, dst) in enumerate((
            (sdev_hbm, sdev_ref), (slist_hbm, slist_ref), (srow_hbm, srow_ref),
            (pdev_hbm, pdev_ref), (plist_hbm, plist_ref), (lengths_hbm, lengths),
        ))
    ]
    for copy in small:
        copy.start()
    for t in range(TILES):
        pltpu.make_async_copy(
            q_hbm.at[:, pl.ds(t * 128, 128)], qbuf.at[0, 0, 0, 0, t], load_sem.at[0]
        ).start()

    def greet(peer, flat, off, back):
        pl.semaphore_signal(barrier, inc=1, device_id=peer, device_id_type=MESH)

    peers.each(greet)
    docs_copy = pltpu.make_async_copy(docs_hbm.at[:, pl.ds(0, ELIG), :], docs, load_sem.at[1])
    docs_copy.start()
    dpre_copy = pltpu.make_async_copy(docs_hbm.at[:, :, pl.ds(0, PREFIX)], dpre, load_sem.at[2])
    dpre_copy.start()
    for copy in small:
        copy.wait()

    dev = iota((QROWS, DEVS), 1)
    sdev = sdev_ref[...]
    scode = (slist_ref[...] * ELIG + srow_ref[...] + 1).astype(F32)
    pdev = pdev_ref[...]
    pcode = (plist_ref[...] + 1).astype(F32)
    lower = (iota((QROWS, QROWS), 1) < iota((QROWS, QROWS), 0)).astype(F32).astype(BF16)
    qnum = iota((QROWS, DEVS), 0).astype(F32) + 1.0

    def table(devs, codes, width):
        got = jnp.zeros((QROWS, DEVS), F32)
        for s in range(width):
            got = got + jnp.where(devs[:, s : s + 1] == dev, codes[:, s : s + 1], 0.0)
        used = jnp.where(got > 0.0, 1.0, 0.0)
        rank = jnp.dot(lower, used.astype(BF16), preferred_element_type=F32)
        return got, jnp.where(used > 0.0, rank, -1.0)

    stab, srank = table(sdev, scode, SHORT)
    ptab, prank = table(pdev, pcode, PROBES)
    krow = iota((16, DEVS), 0)
    slots = jnp.zeros((16, DEVS), F32)
    for base, row_base, tab, rank, cap in (
        (LANE_CODE, LANE_ROW, stab, srank, CAP),
        (LANE_LIST, LANE_PROW, ptab, prank, PCAP),
    ):
        for j in range(cap):
            hit = rank == float(j)
            code = jnp.sum(jnp.where(hit, tab, 0.0), axis=0, keepdims=True) - 1.0
            row = jnp.sum(jnp.where(hit, qnum, 0.0), axis=0, keepdims=True) - 1.0
            slots = jnp.where(krow == base + j, code, slots)
            slots = jnp.where(krow == row_base + j, row, slots)
    slots = jnp.concatenate([slots, jnp.zeros((112, DEVS), F32)], axis=0).T
    ask[...] = slots.astype(I32).reshape(DEVS, 1, DEVS)

    pltpu.make_async_copy(qbuf.at[0, 0, 0, 1], qbuf.at[0, 0, 0, 0], load_sem.at[0]).wait()
    pl.semaphore_wait(barrier, DEVS - 1)
    gather = Gather(qbuf, gsend, grecv, gcross, me)
    gather.begin()
    def exchange(send, recv, number, by_offset):
        def visit(peer, flat, off, back):
            if by_offset:
                src, dst = send.at[off], recv.at[own_number]
            else:
                src, dst = send.at[flat], recv.at[back]
            pltpu.make_async_remote_copy(
                src_ref=src, dst_ref=dst, send_sem=xsend.at[number], recv_sem=xrecv.at[number],
                device_id=peer, device_id_type=MESH,
            ).start()

        peers.each(visit)

    def exchanged(send, recv, number):
        rest = pl.ds(0, DEVS - 1)
        pltpu.make_async_copy(recv.at[rest], recv.at[rest], xrecv.at[number]).wait()
        pltpu.make_async_copy(send.at[rest], send.at[rest], xsend.at[number]).wait()

    exchange(ask, asked, 0, False)

    lane = iota((16, DEVS), 1)

    def read_slots():
        exchanged(ask, asked, 0)
        asked[0] = ask[own_number]
        docs_copy.wait()
        dpre_copy.wait()
        slot_ref[...] = asked[...].reshape(DEVS, DEVS)

    def mark(j):
        doc_number = iota((DEVS, LISTS * ELIG), 1)
        hit = slot_ref[:, LANE_CODE + j : LANE_CODE + j + 1] == doc_number
        oh[pl.ds(j * DEVS, DEVS), :] = jnp.where(hit, 1.0, 0.0).astype(BF16)

    def pick(low, high):
        def body(n, carry):
            cols = pl.ds(pl.multiple_of(n * 256, 256), 256)
            block = docs[:, :, cols].reshape(LISTS * ELIG, 256)
            got = jnp.dot(oh[...], block, preferred_element_type=F32)
            gath[:, :, cols] = got.astype(BF16).reshape(CAP, DEVS, 256)
            return carry

        lax.fori_loop(low, high, body, 0)

    group_row = iota((16, 1), 0)
    group_col = iota((16, 256), 1)

    def queries(g, low, high):
        tiles = [qbuf[g % SIDE, :, :, g // SIDE, t].reshape(256, 128) for t in range(low, high)]
        return jnp.concatenate(tiles, axis=1)

    def column(g, at):
        number = slot_ref[pl.ds(g * 16, 16), at : at + 1]
        return jnp.where(number < 0, -1, group_row * QROWS + number)

    def prefix_scores():
        for g in range(2 * SIDE):
            hits = [jnp.where(column(g, LANE_PROW + p) == group_col, 1.0, 0.0) for p in range(PCAP)]
            hit = jnp.concatenate(hits, axis=0).astype(BF16)
            rows = jnp.dot(hit, queries(g, 0, PREFIX // 128), preferred_element_type=F32)
            norm = jnp.sqrt(1.0 + jnp.sum(rows * rows, axis=1, keepdims=True))
            rows = rows / norm
            for p in range(PCAP):
                psel[pl.ds(p * DEVS + g * 16, 16), :] = rows[p * 16 : (p + 1) * 16, :]
        slot_t = slot_ref[...].astype(F32).T
        lists = jnp.concatenate(
            [slot_t[LANE_LIST + p : LANE_LIST + p + 1, :] for p in range(PCAP)], axis=1
        )
        wanted = psel[...].T.astype(BF16)
        sel[...] = jnp.zeros_like(sel)
        for n in range(LISTS):
            got = jnp.dot(dpre[n], wanted, preferred_element_type=F32)
            sel[...] = jnp.where(lists == float(n), got, sel[...])
        rows_valid = jnp.zeros((1, PCAP * DEVS), I32)
        for n in range(LISTS):
            rows_valid = jnp.where(lists == float(n), lengths[n], rows_valid)
        sub = iota((8, DEVS), 0)
        tops = []
        for p in range(PCAP):
            lanes = pl.ds(p * DEVS, DEVS)
            bound = rows_valid[:, p * DEVS : (p + 1) * DEVS]
            seq = [
                jnp.where(sub + v * 8 < bound, sel[pl.ds(v * 8, 8), lanes], LOW) for v in range(32)
            ]
            seq = sort_down(seq)
            for shift in (4, 2, 1):
                seq = join_rolled(seq, shift, 0)
            for m in range(TOPK // 8):
                block = seq[m * 8]
                for s in range(1, 8):
                    block = jnp.where(sub == s, seq[m * 8 + s], block)
                tops.append(block)
        tops.append(jnp.zeros((DEVS - PCAP * TOPK, DEVS), F32))
        psend[...] = jnp.concatenate(tops, axis=0).T.reshape(DEVS, 1, DEVS)

    def return_prefix():
        exchange(psend, precv, 1, True)

    def merge_prefix():
        exchanged(psend, precv, 1)
        precv[own_number] = psend[0]
        back = precv[...].reshape(DEVS, DEVS).T
        first, second = prank == 0.0, prank == 1.0
        seq = [
            jnp.where(
                first, back[k : k + 1, :], jnp.where(second, back[TOPK + k : TOPK + k + 1, :], LOW)
            )
            for k in range(TOPK)
        ]
        for shift in (64, 32, 16, 8, 4, 2, 1):
            seq = join_rolled(seq, shift, 1)
        best = seq[0]
        for k in range(1, TOPK):
            best = jnp.where(lane == k, seq[k], best)
        out_ref[...] = best

    first, others = gather.parts[:1], gather.parts[1:]
    gather.first_axis(first)
    gather.first_axis(others)
    gather.home_blocks(first)
    gather.home_blocks(others)
    gather.second_axis(first)
    read_slots()
    for j in range(CAP):
        mark(j)
    gather.second_axis(others)
    gather.third_axis_line(first)
    gather.second_axis_end(first)
    pick(0, 2)
    gather.third_axis_line(others)
    gather.third_axis(first, NEAR)
    gather.second_axis_end(others)
    gather.third_axis(first, FAR)
    gather.third_axis_line_end(first)
    pick(2, 4)
    gather.third_axis(others, NEAR)
    gather.third_axis_end(first, NEAR)
    gather.third_axis_end(first, FAR)
    pick(4, 6)
    gather.third_axis(others, FAR)
    gather.wait_partner(0)
    prefix_scores()
    return_prefix()
    gather.third_axis_line_end(others)
    gather.third_axis_end(others, NEAR)
    pick(6, 8)
    gather.third_axis_end(others, FAR)

    def rescore(groups):
        for g in groups:
            left = gath[:, pl.ds(g * 16, 16), :].reshape(CAP * 16, FULL)
            got = lax.dot_general(
                left, queries(g, 0, TILES), (((1,), (1,)), ((), ())), preferred_element_type=F32
            )
            total = jnp.zeros((16, 256), F32)
            for j in range(CAP):
                hit = column(g, LANE_ROW + j) == group_col
                total = total + jnp.where(hit, got[j * 16 : (j + 1) * 16, :], 0.0)
            value = jnp.sum(total, axis=0, keepdims=True)
            for half in range(2):
                rsend[g * 2 + half] = value[:, half * 128 : (half + 1) * 128]
        for g in groups:
            for half, peer in peers.group(g):
                pltpu.make_async_remote_copy(
                    src_ref=rsend.at[g * 2 + half], dst_ref=rrecv.at[own_number],
                    send_sem=xsend.at[2], recv_sem=xrecv.at[2], device_id=peer, device_id_type=MESH,
                ).start()

    rescore((2, 1))
    rescore((3, 0))
    gather.wait_partner(1)
    rescore((6, 5))
    rescore((7, 4))
    gather.drain()
    merge_prefix()
    exchanged(rrecv, rrecv, 2)
    squares = jnp.zeros((QROWS, 128), F32)
    for t in range(TILES):
        value = qbuf[0, 0, 0, 0, t].astype(F32)
        squares = squares + value * value
    full_norm = jnp.sqrt(1.0 + jnp.sum(squares, axis=1, keepdims=True))
    rrecv[own_number] = rsend[0]
    back = rrecv[...].reshape(DEVS, DEVS).T
    other = iota((16, DEVS), 1)
    other_x, other_z = other // 8 % SIDE, other // 2 % SIDE
    place = (me[1] + SIDE - other_x) % 2 * SIDE + (me[2] + SIDE - other_z) % SIDE
    value = jnp.zeros((QROWS, DEVS), F32)
    for n in range(8):
        value = jnp.where(place == n, back[n * 16 : (n + 1) * 16, :], value)
    out = jnp.zeros((QROWS, DEVS), F32)
    for s in range(SHORT):
        one = jnp.sum(jnp.where(sdev[:, s : s + 1] == dev, value, 0.0), axis=1, keepdims=True)
        out = jnp.where(lane == s, one, out)
    out_ref[:, pl.ds(TOPK, SHORT)] = (out / full_norm)[:, :SHORT]


def shards(queries, probe_dev, probe_list, documents, lengths, short_dev, short_list, short_row):
    vmem = pl.BlockSpec(memory_space=pltpu.VMEM)
    anywhere = pl.BlockSpec(memory_space=pl.ANY)
    out = pl.pallas_call(
        kernel,
        name="search",
        out_shape=pltpu.VMEM((QROWS, DEVS), F32),
        in_specs=[anywhere] * 8,
        out_specs=vmem,
        scratch_shapes=[
            pltpu.SMEM((LISTS,), I32),
            pltpu.VMEM((QROWS, SHORT), I32),
            pltpu.VMEM((QROWS, SHORT), I32),
            pltpu.VMEM((QROWS, SHORT), I32),
            pltpu.VMEM((QROWS, PROBES), I32),
            pltpu.VMEM((QROWS, PROBES), I32),
            pltpu.VMEM((SIDE, SIDE, SIDE, 2, TILES, QROWS, 128), BF16),
            pltpu.VMEM((LISTS, ELIG, FULL), BF16),
            pltpu.VMEM((LISTS, ROWS, PREFIX), BF16),
            pltpu.VMEM((CAP, DEVS, FULL), BF16),
            pltpu.VMEM((CAP * DEVS, LISTS * ELIG), BF16),
            pltpu.VMEM((ROWS, PCAP * DEVS), F32),
            pltpu.VMEM((DEVS, DEVS), I32),
            pltpu.VMEM((PCAP * DEVS, PREFIX), F32),
            pltpu.VMEM((DEVS, 1, DEVS), I32),
            pltpu.VMEM((DEVS, 1, DEVS), I32),
            pltpu.VMEM((DEVS, 1, DEVS), F32),
            pltpu.VMEM((DEVS, 1, DEVS), F32),
            pltpu.VMEM((4 * SIDE, 1, DEVS), F32),
            pltpu.VMEM((DEVS, 1, DEVS), F32),
            pltpu.SemaphoreType.DMA((6,)),
            pltpu.SemaphoreType.DMA((3,)),
            pltpu.SemaphoreType.DMA,
            pltpu.SemaphoreType.DMA((RINGS * 3 * len(PARTS),)),
            pltpu.SemaphoreType.DMA((2,)),
            pltpu.SemaphoreType.DMA((3,)),
            pltpu.SemaphoreType.DMA((3,)),
        ],
        compiler_params=pltpu.CompilerParams(
            collective_id=0, has_side_effects=True, vmem_limit_bytes=60 * 1024 * 1024
        ),
    )(queries, documents, lengths, short_dev, short_list, short_row, probe_dev, probe_list)
    return out[:, :TOPK], out[:, TOPK : TOPK + SHORT]


def solution(mesh):
    spread = P(("gx", "gy"), None)
    in_specs = (spread, spread, spread, P(("gx", "gy"), None, None), P(("gx", "gy")), spread, spread, spread)
    return jax.shard_map(shards, mesh=mesh, in_specs=in_specs, out_specs=(spread, spread), check_vma=False)
```

```python
import jax
import jax.numpy as jnp
from jax import lax
from jax.experimental import pallas as pl
from jax.experimental.pallas import tpu as pltpu
from jax.sharding import PartitionSpec as P

MESH = pl.DeviceIdType.MESH
SIDE = 4
DEVS = 128
QROWS = 16
LISTS = 16
ROWS = 256
ELIG = 96
PREFIX = 256
FULL = 2048
TILES = FULL // 128
CAP = 5
PCAP = 2
TOPK = 32
SHORT = 32
PROBES = 16
LOW = -1e30
PARTS = ((0, 2, 2), (2, 7, 0), (7, 12, 1), (12, 16, 2))
F32 = jnp.float32
BF16 = jnp.bfloat16
I32 = jnp.int32
LANE_CODE, LANE_ROW, LANE_LIST, LANE_PROW = 0, 5, 10, 12


def iota(shape, axis):
    return lax.broadcasted_iota(I32, shape, axis)


def merge_down(seq):
    seq = list(seq)
    step = len(seq) // 2
    while step:
        for i in range(len(seq)):
            if not i & step:
                a, b = seq[i], seq[i + step]
                seq[i], seq[i + step] = jnp.maximum(a, b), jnp.minimum(a, b)
        step //= 2
    return seq


def sort_down(seq):
    if len(seq) == 1:
        return list(seq)
    half = len(seq) // 2
    return merge_down(sort_down(seq[:half]) + sort_down(seq[half:])[::-1])


def join_rolled(seq, shift, axis):
    count = len(seq)
    other = [pltpu.roll(v, shift, axis) for v in seq]
    return merge_down([jnp.maximum(seq[i], other[count - 1 - i]) for i in range(count)])


def coords():
    gx, gy = lax.axis_index("gx"), lax.axis_index("gy")
    return gx // SIDE, gx % SIDE, gy // 2, gy % 2


def device_of(y, x, z, c):
    return (y * SIDE + x, z * 2 + c)


FAR_FIRST = (2, 1, 3, 0)
BLOCKS = sorted(
    ((y, x, z) for y in range(SIDE) for x in range(SIDE) for z in range(SIDE)),
    key=lambda b: (min(2, sum(v == 2 for v in b)), b),
)
CHIPS = len(BLOCKS)
HALF = CHIPS // 2
WAVES = ((0, 27), (27, 54), (54, 64))
WAVE_ROWS = (4, 4, 2)
EVERY, REST = slice(0, SIDE), slice(1, SIDE)
NEAR, FAR = (("C2", 3), ("C3", 1)), (("C4", 2),)
NEAR_SEM = dict(A="A", B0="B0", C0="C0", B1="B1", C1="C1", C2="C23", C3="C23", C4="C4")
END_SEM = dict(A="A", B0="B_", B1="B_", C0="C01_", C1="C01_", C2="C23_", C3="C23_", C4="C4_")
STRAIGHT_FIRST, STRAIGHT = ("A", "B0", "B1", "C4"), ("A",)


class Peers:
    def __init__(self, me):
        rows = [(me[0] + d) % SIDE * SIDE for d in range(SIDE)]
        xs = [(me[1] + d) % SIDE for d in range(SIDE)]
        zs = [(me[2] + d) % SIDE * 2 for d in range(SIDE)]
        self.gxs = [[row + x for x in xs] for row in rows]
        self.gys = [[z + me[3], z + 1 - me[3]] for z in zs]

    def at(self, off):
        y, x, z = BLOCKS[off % CHIPS]
        return self.gxs[y][x], self.gys[z][off // CHIPS]

    def each(self, visit, near_half_first=False):
        def order(off):
            return near_half_first and off % CHIPS // HALF, -sum(min(v, SIDE - v) for v in BLOCKS[off % CHIPS])

        for off in sorted(range(1, DEVS), key=order):
            gx, gy = self.at(off)
            back = tuple((SIDE - v) % SIDE for v in BLOCKS[off % CHIPS])
            visit((gx, gy), gx * 8 + gy, off, off // CHIPS * CHIPS + BLOCKS.index(back))


class Gather:
    def __init__(self, qbuf, send_sem, recv_sem, cross_sem, me):
        self.qbuf, self.send_sem, self.recv_sem = qbuf, send_sem, recv_sem
        self.cross_sem, self.me = cross_sem, me
        self.sems = {}
        y, x, z, c = me
        self.partner = device_of(y, x, z, 1 - c)
        self.peers = {}
        for axis in range(3):
            for step in (1, 2, 3):
                place = list(me)
                place[axis] = (place[axis] + step) % SIDE
                self.peers[axis, step] = device_of(*place)

    def view(self, where, tiles, core=0):
        return self.qbuf.at[where[0], where[1], where[2], core, tiles]

    def start(self, src, dst, peer, sem):
        pltpu.make_async_remote_copy(
            src_ref=src, dst_ref=dst, send_sem=self.send_sem, recv_sem=sem,
            device_id=peer, device_id_type=MESH,
        ).start()

    def sem(self, part, name):
        key = part["number"], name
        if key not in self.sems:
            self.sems[key] = len(self.sems)
        return self.recv_sem.at[self.sems[key]]

    def slot(self, part, name, value, tiles=None):
        unit, axis = part[name]
        where = list(unit)
        where[axis] = value
        return self.view(where, tiles or part["tiles"])

    def ring_start(self, part, name, order, a, b):
        axis = part["axes"][order]
        part[name] = self.unit(part, a, b, 0), axis
        own = self.slot(part, name, 0)
        near = self.sem(part, NEAR_SEM[name])
        self.start(own, self.slot(part, name, 3), self.peers[axis, 1], near)
        self.start(own, self.slot(part, name, 1), self.peers[axis, 3], near)
        if self.straight(part, name):
            self.start(own, self.slot(part, name, 2), self.peers[axis, 2], self.sem(part, END_SEM[name]))

    def straight(self, part, name):
        return name in (STRAIGHT_FIRST if part["number"] == 0 else STRAIGHT)

    def wait(self, ref, sem):
        pltpu.make_async_copy(ref, ref, sem).wait()

    def near(self, part, names):
        self.wait(self.as_many(part, names, slice(1, 3)), self.sem(part, NEAR_SEM[names[0]]))
        tiles = part["tiles"]
        middle = (tiles.start + tiles.stop) // 2
        for name in names:
            if self.straight(part, name):
                continue
            end = self.sem(part, END_SEM[name])
            axis = part[name][1]
            for value, step, piece in ((3, 1, slice(tiles.start, middle)), (1, 3, slice(middle, tiles.stop))):
                self.start(
                    self.slot(part, name, value, piece), self.slot(part, name, 2, piece), self.peers[axis, step], end
                )

    def end(self, part, names):
        self.wait(self.as_many(part, names, 2), self.sem(part, END_SEM[names[0]]))

    def as_many(self, part, names, value):
        unit, axis = part[names[0]]
        where = list(unit)
        where[axis] = value
        if names in (("B0", "B1"), ("C0", "C1")):
            where[part["axes"][0]] = EVERY
        elif len(names) > 1:
            where[part["axes"][1]] = slice(0, len(names))
        return self.view(where, part["tiles"])

    def across(self, part, where, wave):
        tiles = part["tiles"]
        sem = self.cross_sem.at[wave + 1 if part["number"] or wave == 0 else 0]
        self.start(self.view(where, tiles, 0), self.view(where, tiles, 1), self.partner, sem)

    def unit(self, part, a, b, c):
        where = [0, 0, 0]
        for axis, value in zip(part["axes"], (a, b, c)):
            where[axis] = value
        return where

    def to_c(self, part, name, a, b):
        self.ring_start(part, name, 2, a, b)
        self.across(part, self.unit(part, a, b, 0), int(b == 2))

    def begin(self):
        self.parts = []
        for number, (low, high, first) in enumerate(PARTS):
            axes = (first, (first + 1) % 3, (first + 2) % 3)
            self.parts.append(dict(number=number, axes=axes, tiles=slice(low, high)))
        for order, name in enumerate(("A", "B0", "C0")):
            for part in self.parts:
                self.ring_start(part, name, order, 0, 0)
        for part in self.parts:
            self.across(part, [0, 0, 0], 0)

    def first_axis(self, parts):
        for part in parts:
            self.wait(self.as_many(part, ("A",), REST), self.sem(part, "A"))
            self.ring_start(part, "B1", 1, REST, 0)

    def home_blocks(self, parts):
        for name in ("B0", "C0"):
            for part in parts:
                self.near(part, (name,))
        for part in parts:
            self.to_c(part, "C1", REST, 0)

    def second_axis(self, parts):
        for part in parts:
            self.near(part, ("B1",))
        for part in parts:
            self.to_c(part, "C2", EVERY, 3)
            self.to_c(part, "C3", EVERY, 1)

    def second_axis_end(self, parts):
        for part in parts:
            self.end(part, ("B0", "B1"))
            self.to_c(part, "C4", EVERY, 2)

    def third_axis_line(self, parts):
        for part in parts:
            self.near(part, ("C1",))
            self.across(part, self.unit(part, EVERY, 0, 3), 0)
            self.across(part, self.unit(part, EVERY, 0, 1), 0)

    def third_axis(self, parts, pairs):
        for part in parts:
            self.near(part, tuple(name for name, _ in pairs))
            for _, b in pairs:
                self.across(part, self.unit(part, EVERY, b, 3), int(b == 2))
                self.across(part, self.unit(part, EVERY, b, 1), int(b == 2))

    def third_axis_line_end(self, parts):
        for part in parts:
            self.end(part, ("C0", "C1"))
            self.across(part, self.unit(part, EVERY, 0, 2), 1)

    def third_axis_end(self, parts, pairs):
        for part in parts:
            self.end(part, tuple(name for name, _ in pairs))
            for _, b in pairs:
                self.across(part, self.unit(part, EVERY, b, 2), 1 + int(b == 2))

    def wait_partner_first(self):
        low = PARTS[0][1]
        assert 28 * low == 4 * (TILES - low)
        self.wait(self.qbuf.at[:, 0, 0, 1, slice(low, TILES)], self.cross_sem.at[0])

    def wait_partner(self, wave):
        ys, zs = (slice(0, 3), slice(0, 3), slice(0, 1))[wave], (slice(0, 3), slice(0, 2), slice(0, 1))[wave]
        ref = self.qbuf.at[:, ys, zs, 1, slice(PARTS[0][1] if wave else 0, TILES)]
        self.wait(ref, self.cross_sem.at[wave + 1])

    def drain(self):
        rest = slice(1, SIDE)
        for ref in (
            self.qbuf.at[rest], self.qbuf.at[0, rest], self.qbuf.at[0, 0, rest], self.qbuf.at[0, 0, 0, 1]
        ):
            pltpu.make_async_copy(ref, ref, self.send_sem).wait()


def kernel(
    q_hbm, docs_hbm, lengths_hbm, sdev_hbm, slist_hbm, srow_hbm, pdev_hbm, plist_hbm,
    out_ref,
    lengths, sdev_ref, slist_ref, srow_ref, pdev_ref, plist_ref,
    qbuf, docs, dpre, gath, oh, sel, slot_ref, psel, ask, asked, psend, precv, rsend, rrecv,
    known, small_sem, load_sem, gsend, grecv, gcross, xsend, xrecv,
):
    me = coords()
    own_number = (me[0] * SIDE + me[1]) * 8 + me[2] * 2 + me[3]
    peers = Peers(me)
    barrier = pltpu.get_barrier_semaphore()
    small = [
        pltpu.make_async_copy(src, dst, small_sem.at[n])
        for n, (src, dst) in enumerate((
            (sdev_hbm, sdev_ref), (slist_hbm, slist_ref), (srow_hbm, srow_ref),
            (pdev_hbm, pdev_ref), (plist_hbm, plist_ref), (lengths_hbm, lengths),
        ))
    ]
    for copy in small:
        copy.start()

    gather = Gather(qbuf, gsend, grecv, gcross, me)
    lines = [[gather.peers[axis, step] for step in (2, 1, 3)] for axis in range(3)]

    def tell(sem, them):
        for peer in them:
            pl.semaphore_signal(sem, inc=1, device_id=peer, device_id_type=MESH)

    others = [(gx, gather.partner[1]) for gx, _ in lines[0]] + [gather.partner]
    tell(barrier, lines[0] + others + lines[1] + lines[2])

    for t in range(TILES):
        pltpu.make_async_copy(
            q_hbm.at[:, pl.ds(t * 128, 128)], qbuf.at[0, 0, 0, 0, t], load_sem.at[0]
        ).start()

    docs_copy = pltpu.make_async_copy(docs_hbm.at[:, pl.ds(0, ELIG), :], docs, load_sem.at[1])
    docs_copy.start()
    dpre_copy = pltpu.make_async_copy(docs_hbm.at[:, :, pl.ds(0, PREFIX)], dpre, load_sem.at[2])
    dpre_copy.start()
    for copy in small:
        copy.wait()

    dev = iota((QROWS, DEVS), 1)
    sdev = sdev_ref[...]
    scode = (slist_ref[...] * ELIG + srow_ref[...] + 1).astype(F32)
    pdev = pdev_ref[...]
    pcode = (plist_ref[...] + 1).astype(F32)
    lower = (iota((QROWS, QROWS), 1) < iota((QROWS, QROWS), 0)).astype(F32).astype(BF16)
    qnum = iota((QROWS, DEVS), 0).astype(F32) + 1.0

    def table(devs, codes, width):
        got = jnp.zeros((QROWS, DEVS), F32)
        for s in range(width):
            got = got + jnp.where(devs[:, s : s + 1] == dev, codes[:, s : s + 1], 0.0)
        used = jnp.where(got > 0.0, 1.0, 0.0)
        rank = jnp.dot(lower, used.astype(BF16), preferred_element_type=F32)
        return got, jnp.where(used > 0.0, rank, -1.0)

    stab, srank = table(sdev, scode, SHORT)
    ptab, prank = table(pdev, pcode, PROBES)
    krow = iota((16, DEVS), 0)
    slots = jnp.zeros((16, DEVS), F32)
    for base, row_base, tab, rank, cap in (
        (LANE_CODE, LANE_ROW, stab, srank, CAP),
        (LANE_LIST, LANE_PROW, ptab, prank, PCAP),
    ):
        for j in range(cap):
            hit = rank == float(j)
            code = jnp.sum(jnp.where(hit, tab, 0.0), axis=0, keepdims=True) - 1.0
            row = jnp.sum(jnp.where(hit, qnum, 0.0), axis=0, keepdims=True) - 1.0
            slots = jnp.where(krow == base + j, code, slots)
            slots = jnp.where(krow == row_base + j, row, slots)
    slots = jnp.concatenate([slots, jnp.zeros((112, DEVS), F32)], axis=0).T
    ask[...] = slots.astype(I32).reshape(DEVS, 1, DEVS)

    pltpu.make_async_copy(qbuf.at[0, 0, 0, 1], qbuf.at[0, 0, 0, 0], load_sem.at[0]).wait()
    pl.semaphore_wait(barrier, 13)
    tell(known.at[0], lines[1])
    gather.begin()
    def exchange_rows(src, dst, peer, number):
        pltpu.make_async_remote_copy(
            src_ref=src, dst_ref=dst, send_sem=xsend.at[number], recv_sem=xrecv.at[number],
            device_id=peer, device_id_type=MESH,
        ).start()

    def exchanged(send, recv, number, rows):
        some = pl.ds(0, rows)
        pltpu.make_async_copy(recv.at[some], recv.at[some], xrecv.at[number]).wait()
        pltpu.make_async_copy(send.at[some], send.at[some], xsend.at[number]).wait()

    def ask_peer(peer, flat, off, back):
        exchange_rows(ask.at[flat], asked.at[back], peer, back % CHIPS // HALF)


    lane = iota((16, DEVS), 1)

    def read_slots(half):
        exchanged(ask, asked, half, DEVS // 2 - (half == 0))
        if half == 0:
            asked[0] = ask[own_number]
        for core in range(2):
            here = pl.ds(core * CHIPS + half * HALF, HALF)
            slot_ref[here] = asked[here].reshape(HALF, DEVS)
        doc_number = iota((HALF, LISTS * ELIG), 1)
        for j in range(CAP):
            for core in range(2):
                here = pl.ds(core * CHIPS + half * HALF, HALF)
                hit = slot_ref[here, LANE_CODE + j : LANE_CODE + j + 1] == doc_number
                oh[half, pl.ds((j * 2 + core) * HALF, HALF), :] = jnp.where(hit, 1.0, 0.0).astype(BF16)

    def pick(half, low, high):
        def body(n, carry):
            cols = pl.ds(pl.multiple_of(n * 256, 256), 256)
            block = docs[:, :, cols].reshape(LISTS * ELIG, 256)
            got = jnp.dot(oh[half], block, preferred_element_type=F32)
            gath[:, :, pl.ds(half * HALF, HALF), cols] = got.astype(BF16).reshape(CAP, 2, HALF, 256)
            return carry

        lax.fori_loop(low, high, body, 0, unroll=2)

    group_row = iota((16, 1), 0)
    group_col = iota((16, 256), 1)

    def blocks(start, stop, low, high):
        places = [(*BLOCKS[off % CHIPS], off // CHIPS) for off in range(start, stop)]
        tiles = [
            jnp.concatenate([qbuf[y, x, z, c, t] for y, x, z, c in places], axis=0)
            for t in range(low, high)
        ]
        return jnp.concatenate(tiles, axis=1)

    def queries(g, low, high):
        return blocks(g * 16, g * 16 + 16, low, high)

    def column(g, at):
        number = slot_ref[pl.ds(g * 16, 16), at : at + 1]
        return jnp.where(number < 0, -1, group_row * QROWS + number)

    def prefix_scores():
        for g in range(2 * SIDE):
            hits = [jnp.where(column(g, LANE_PROW + p) == group_col, 1.0, 0.0) for p in range(PCAP)]
            hit = jnp.concatenate(hits, axis=0).astype(BF16)
            rows = jnp.dot(hit, queries(g, 0, PREFIX // 128), preferred_element_type=F32)
            norm = jnp.sqrt(1.0 + jnp.sum(rows * rows, axis=1, keepdims=True))
            rows = rows / norm
            for p in range(PCAP):
                psel[pl.ds(p * DEVS + g * 16, 16), :] = rows[p * 16 : (p + 1) * 16, :]
        slot_t = slot_ref[...].astype(F32).T
        lists = jnp.concatenate(
            [slot_t[LANE_LIST + p : LANE_LIST + p + 1, :] for p in range(PCAP)], axis=1
        )
        wanted = psel[...].T.astype(BF16)
        sel[...] = jnp.zeros_like(sel)
        for n in range(LISTS):
            got = jnp.dot(dpre[n], wanted, preferred_element_type=F32)
            sel[...] = jnp.where(lists == float(n), got, sel[...])
        rows_valid = jnp.zeros((1, PCAP * DEVS), I32)
        for n in range(LISTS):
            rows_valid = jnp.where(lists == float(n), lengths[n], rows_valid)
        sub = iota((8, DEVS), 0)
        tops = []
        for p in range(PCAP):
            lanes = pl.ds(p * DEVS, DEVS)
            bound = rows_valid[:, p * DEVS : (p + 1) * DEVS]
            seq = [
                jnp.where(sub + v * 8 < bound, sel[pl.ds(v * 8, 8), lanes], LOW) for v in range(32)
            ]
            seq = sort_down(seq)
            for shift in (4, 2, 1):
                seq = join_rolled(seq, shift, 0)
            for m in range(TOPK // 8):
                block = seq[m * 8]
                for s in range(1, 8):
                    block = jnp.where(sub == s, seq[m * 8 + s], block)
                tops.append(block)
        tops.append(jnp.zeros((DEVS - PCAP * TOPK, DEVS), F32))
        psend[...] = jnp.concatenate(tops, axis=0).T.reshape(DEVS, 1, DEVS)

    def return_prefix():
        peers.each(lambda peer, flat, off, back: exchange_rows(psend.at[off], precv.at[own_number], peer, 2))

    def merge_prefix():
        exchanged(psend, precv, 2, DEVS - 1)
        precv[own_number] = psend[0]
        back = precv[...].reshape(DEVS, DEVS).T
        first, second = prank == 0.0, prank == 1.0
        seq = [
            jnp.where(
                first, back[k : k + 1, :], jnp.where(second, back[TOPK + k : TOPK + k + 1, :], LOW)
            )
            for k in range(TOPK)
        ]
        for shift in (64, 32, 16, 8, 4, 2, 1):
            seq = join_rolled(seq, shift, 1)
        best = seq[0]
        for k in range(1, TOPK):
            best = jnp.where(lane == k, seq[k], best)
        out_ref[...] = best

    def rescore(wave, core):
        start, stop = WAVES[wave]
        low, high = start // 16 * 16, -(-stop // 16) * 16
        rows, cols = high - low, (stop - start) * QROWS
        left = gath[:, core, pl.ds(low, rows), :].reshape(CAP * rows, FULL)
        start, stop, low = start + core * CHIPS, stop + core * CHIPS, low + core * CHIPS
        got = lax.dot_general(
            left, blocks(start, stop, 0, TILES), (((1,), (1,)), ((), ())), preferred_element_type=F32
        )
        base = (iota((rows, 1), 0) + (low - start)) * QROWS
        col = iota((rows, cols), 1)
        total = jnp.zeros((rows, cols), F32)
        for j in range(CAP):
            number = slot_ref[pl.ds(low, rows), LANE_ROW + j : LANE_ROW + j + 1]
            hit = jnp.where(number < 0, -1, base + number) == col
            total = total + jnp.where(hit, got[j * rows : (j + 1) * rows, :], 0.0)
        value = jnp.sum(total, axis=0, keepdims=True)
        rest = WAVE_ROWS[wave] * 128 - cols
        value = jnp.concatenate([value, jnp.zeros((1, rest), F32)], axis=1)
        to = core * sum(WAVE_ROWS) + sum(WAVE_ROWS[:wave])
        for n in range(WAVE_ROWS[wave]):
            rsend[to + n] = value[:, n * 128 : (n + 1) * 128]
        for off in range(start, stop):
            if off:
                exchange_rows(rsend.at[to + (off - start) // 8], rrecv.at[own_number], peers.at(off), 3)

    first, others = gather.parts[:1], gather.parts[1:]
    pl.semaphore_wait(known.at[0], 3)
    tell(known.at[1], lines[2])
    gather.first_axis(first)
    gather.first_axis(others)
    pl.semaphore_wait(known.at[1], 3)
    peers.each(ask_peer, near_half_first=True)
    gather.home_blocks(first)
    gather.home_blocks(others)
    docs_copy.wait()
    dpre_copy.wait()
    gather.second_axis(first)
    gather.second_axis(others)
    gather.third_axis_line(first)
    gather.second_axis_end(first)
    gather.third_axis_line(others)
    read_slots(0)
    pick(0, 0, 2)
    gather.second_axis_end(others)
    gather.third_axis(first, NEAR)
    read_slots(1)
    pick(0, 2, 8)
    gather.third_axis(others, NEAR)
    pick(1, 0, 4)
    gather.third_axis(first, FAR)
    gather.third_axis_line_end(first)
    pick(1, 4, 8)
    gather.third_axis(others, FAR)
    gather.third_axis_end(first, NEAR)
    gather.third_axis_end(first, FAR)
    rescore(0, 0)
    gather.wait_partner(0)
    rescore(0, 1)
    gather.third_axis_line_end(others)
    gather.third_axis_end(others, NEAR)
    gather.wait_partner_first()
    prefix_scores()
    return_prefix()
    gather.third_axis_end(others, FAR)
    rescore(1, 0)
    rescore(2, 0)
    gather.wait_partner(1)
    rescore(1, 1)
    gather.wait_partner(2)
    rescore(2, 1)
    gather.drain()
    merge_prefix()
    exchanged(rrecv, rrecv, 3, DEVS - 1)
    squares = jnp.zeros((QROWS, 128), F32)
    for t in range(TILES):
        value = qbuf[0, 0, 0, 0, t].astype(F32)
        squares = squares + value * value
    full_norm = jnp.sqrt(1.0 + jnp.sum(squares, axis=1, keepdims=True))
    rrecv[own_number] = rsend[0]
    back = rrecv[...].reshape(DEVS, DEVS).T
    other = iota((16, DEVS), 1)
    seen = (me[0] + SIDE - other // 32) % SIDE * 16 + (me[1] + SIDE - other // 8 % SIDE) % SIDE * 4
    seen = seen + (me[2] + SIDE - other // 2 % SIDE) % SIDE
    place = jnp.zeros((QROWS, DEVS), I32)
    for low, high in WAVES:
        for n in range(low, high):
            y, x, z = BLOCKS[n]
            place = jnp.where(seen == y * 16 + x * 4 + z, (n - low) % 8, place)
    value = jnp.zeros((QROWS, DEVS), F32)
    for n in range(8):
        value = jnp.where(place == n, back[n * 16 : (n + 1) * 16, :], value)
    out = jnp.zeros((QROWS, DEVS), F32)
    for s in range(SHORT):
        one = jnp.sum(jnp.where(sdev[:, s : s + 1] == dev, value, 0.0), axis=1, keepdims=True)
        out = jnp.where(lane == s, one, out)
    out_ref[:, pl.ds(TOPK, SHORT)] = (out / full_norm)[:, :SHORT]


def shards(queries, probe_dev, probe_list, documents, lengths, short_dev, short_list, short_row):
    vmem = pl.BlockSpec(memory_space=pltpu.VMEM)
    anywhere = pl.BlockSpec(memory_space=pl.ANY)
    out = pl.pallas_call(
        kernel,
        name="search",
        out_shape=pltpu.VMEM((QROWS, DEVS), F32),
        in_specs=[anywhere] * 8,
        out_specs=vmem,
        scratch_shapes=[
            pltpu.SMEM((LISTS,), I32),
            pltpu.VMEM((QROWS, SHORT), I32),
            pltpu.VMEM((QROWS, SHORT), I32),
            pltpu.VMEM((QROWS, SHORT), I32),
            pltpu.VMEM((QROWS, PROBES), I32),
            pltpu.VMEM((QROWS, PROBES), I32),
            pltpu.VMEM((SIDE, SIDE, SIDE, 2, TILES, QROWS, 128), BF16),
            pltpu.VMEM((LISTS, ELIG, FULL), BF16),
            pltpu.VMEM((LISTS, ROWS, PREFIX), BF16),
            pltpu.VMEM((CAP, 2, CHIPS, FULL), BF16),
            pltpu.VMEM((2, CAP * CHIPS, LISTS * ELIG), BF16),
            pltpu.VMEM((ROWS, PCAP * DEVS), F32),
            pltpu.VMEM((DEVS, DEVS), I32),
            pltpu.VMEM((PCAP * DEVS, PREFIX), F32),
            pltpu.VMEM((DEVS, 1, DEVS), I32),
            pltpu.VMEM((DEVS, 1, DEVS), I32),
            pltpu.VMEM((DEVS, 1, DEVS), F32),
            pltpu.VMEM((DEVS, 1, DEVS), F32),
            pltpu.VMEM((2 * sum(WAVE_ROWS), 1, DEVS), F32),
            pltpu.VMEM((DEVS, 1, DEVS), F32),
            pltpu.SemaphoreType.REGULAR((2,)),
            pltpu.SemaphoreType.DMA((6,)),
            pltpu.SemaphoreType.DMA((3,)),
            pltpu.SemaphoreType.DMA,
            pltpu.SemaphoreType.DMA((11 * len(PARTS),)),
            pltpu.SemaphoreType.DMA((4,)),
            pltpu.SemaphoreType.DMA((4,)),
            pltpu.SemaphoreType.DMA((4,)),
        ],
        compiler_params=pltpu.CompilerParams(
            collective_id=0, has_side_effects=True, vmem_limit_bytes=60 * 1024 * 1024
        ),
    )(queries, documents, lengths, short_dev, short_list, short_row, probe_dev, probe_list)
    return out[:, :TOPK], out[:, TOPK : TOPK + SHORT]


def solution(mesh):
    spread = P(("gx", "gy"), None)
    in_specs = (spread, spread, spread, P(("gx", "gy"), None, None), P(("gx", "gy")), spread, spread, spread)
    return jax.shard_map(shards, mesh=mesh, in_specs=in_specs, out_specs=(spread, spread), check_vma=False)
```

```python
import jax
import jax.numpy as jnp
from jax import lax
from jax.experimental import pallas as pl
from jax.experimental.pallas import tpu as pltpu
from jax.sharding import PartitionSpec as P

MESH = pl.DeviceIdType.MESH
SIDE = 4
DEVS = 128
QROWS = 16
LISTS = 16
ROWS = 256
ELIG = 96
PREFIX = 256
FULL = 2048
TILES = FULL // 128
CAP = 5
PCAP = 2
TOPK = 32
SHORT = 32
PROBES = 16
LOW = -1e30
PARTS = ((0, 2, 2), (2, 7, 0), (7, 12, 1), (12, 16, 2))
F32 = jnp.float32
BF16 = jnp.bfloat16
I32 = jnp.int32
LANE_CODE, LANE_ROW, LANE_LIST, LANE_PROW = 0, 5, 10, 12


def iota(shape, axis):
    return lax.broadcasted_iota(I32, shape, axis)


def merge_down(seq):
    seq = list(seq)
    step = len(seq) // 2
    while step:
        for i in range(len(seq)):
            if not i & step:
                a, b = seq[i], seq[i + step]
                seq[i], seq[i + step] = jnp.maximum(a, b), jnp.minimum(a, b)
        step //= 2
    return seq


def sort_down(seq):
    if len(seq) == 1:
        return list(seq)
    half = len(seq) // 2
    return merge_down(sort_down(seq[:half]) + sort_down(seq[half:])[::-1])


def join_rolled(seq, shift, axis):
    count = len(seq)
    other = [pltpu.roll(v, shift, axis) for v in seq]
    return merge_down([jnp.maximum(seq[i], other[count - 1 - i]) for i in range(count)])


def coords():
    gx, gy = lax.axis_index("gx"), lax.axis_index("gy")
    return gx // SIDE, gx % SIDE, gy // 2, gy % 2


def device_of(y, x, z, c):
    return (y * SIDE + x, z * 2 + c)


FAR_FIRST = (2, 1, 3, 0)
BLOCKS = sorted(
    ((y, x, z) for y in range(SIDE) for x in range(SIDE) for z in range(SIDE)),
    key=lambda b: (min(2, sum(v == 2 for v in b)), b),
)
CHIPS = len(BLOCKS)
HALF = CHIPS // 2
WAVES = ((0, 27), (27, 54), (54, 64))
WAVE_ROWS = (4, 4, 2)
EVERY, REST = slice(0, SIDE), slice(1, SIDE)
NEAR, FAR = (("C2", 3), ("C3", 1)), (("C4", 2),)
NEAR_SEM = dict(A="A", B0="B0", C0="C0", B1="B1", C1="C1", C2="C23", C3="C23", C4="C4")
END_SEM = dict(A="A", B0="B_", B1="B_", C0="C01_", C1="C01_", C2="C23_", C3="C23_", C4="C4_")
STRAIGHT_FIRST, STRAIGHT = ("A", "B0", "B1", "C4"), ("A",)


class Peers:
    def __init__(self, me):
        rows = [(me[0] + d) % SIDE * SIDE for d in range(SIDE)]
        xs = [(me[1] + d) % SIDE for d in range(SIDE)]
        zs = [(me[2] + d) % SIDE * 2 for d in range(SIDE)]
        self.gxs = [[row + x for x in xs] for row in rows]
        self.gys = [[z + me[3], z + 1 - me[3]] for z in zs]

    def at(self, off):
        y, x, z = BLOCKS[off % CHIPS]
        return self.gxs[y][x], self.gys[z][off // CHIPS]

    def each(self, visit, near_half_first=False):
        def order(off):
            return near_half_first and off % CHIPS // HALF, -sum(min(v, SIDE - v) for v in BLOCKS[off % CHIPS])

        for off in sorted(range(1, DEVS), key=order):
            gx, gy = self.at(off)
            back = tuple((SIDE - v) % SIDE for v in BLOCKS[off % CHIPS])
            visit((gx, gy), gx * 8 + gy, off, off // CHIPS * CHIPS + BLOCKS.index(back))


class Gather:
    def __init__(self, qbuf, send_sem, recv_sem, cross_sem, me):
        self.qbuf, self.send_sem, self.recv_sem = qbuf, send_sem, recv_sem
        self.cross_sem, self.me = cross_sem, me
        self.sems = {}
        y, x, z, c = me
        self.partner = device_of(y, x, z, 1 - c)
        self.peers = {}
        for axis in range(3):
            for step in (1, 2, 3):
                place = list(me)
                place[axis] = (place[axis] + step) % SIDE
                self.peers[axis, step] = device_of(*place)

    def view(self, where, tiles, core=0):
        return self.qbuf.at[where[0], where[1], where[2], core, tiles]

    def start(self, src, dst, peer, sem):
        pltpu.make_async_remote_copy(
            src_ref=src, dst_ref=dst, send_sem=self.send_sem, recv_sem=sem,
            device_id=peer, device_id_type=MESH,
        ).start()

    def sem(self, part, name):
        key = part["number"], name
        if key not in self.sems:
            self.sems[key] = len(self.sems)
        return self.recv_sem.at[self.sems[key]]

    def slot(self, part, name, value, tiles=None):
        unit, axis = part[name]
        where = list(unit)
        where[axis] = value
        return self.view(where, tiles or part["tiles"])

    def ring_start(self, part, name, order, a, b):
        axis = part["axes"][order]
        part[name] = self.unit(part, a, b, 0), axis
        own = self.slot(part, name, 0)
        near = self.sem(part, NEAR_SEM[name])
        self.start(own, self.slot(part, name, 3), self.peers[axis, 1], near)
        self.start(own, self.slot(part, name, 1), self.peers[axis, 3], near)
        if self.straight(part, name):
            self.start(own, self.slot(part, name, 2), self.peers[axis, 2], self.sem(part, END_SEM[name]))

    def straight(self, part, name):
        return name in (STRAIGHT_FIRST if part["number"] == 0 else STRAIGHT)

    def wait(self, ref, sem):
        pltpu.make_async_copy(ref, ref, sem).wait()

    def near(self, part, names):
        self.wait(self.as_many(part, names, slice(1, 3)), self.sem(part, NEAR_SEM[names[0]]))
        tiles = part["tiles"]
        middle = (tiles.start + tiles.stop) // 2
        for name in names:
            if self.straight(part, name):
                continue
            end = self.sem(part, END_SEM[name])
            axis = part[name][1]
            for value, step, piece in ((3, 1, slice(tiles.start, middle)), (1, 3, slice(middle, tiles.stop))):
                self.start(
                    self.slot(part, name, value, piece), self.slot(part, name, 2, piece), self.peers[axis, step], end
                )

    def end(self, part, names):
        self.wait(self.as_many(part, names, 2), self.sem(part, END_SEM[names[0]]))

    def as_many(self, part, names, value):
        unit, axis = part[names[0]]
        where = list(unit)
        where[axis] = value
        if names in (("B0", "B1"), ("C0", "C1")):
            where[part["axes"][0]] = EVERY
        elif len(names) > 1:
            where[part["axes"][1]] = slice(0, len(names))
        return self.view(where, part["tiles"])

    def across(self, part, where, wave):
        tiles = part["tiles"]
        sem = self.cross_sem.at[wave + 1 if part["number"] or wave == 0 else 0]
        self.start(self.view(where, tiles, 0), self.view(where, tiles, 1), self.partner, sem)

    def unit(self, part, a, b, c):
        where = [0, 0, 0]
        for axis, value in zip(part["axes"], (a, b, c)):
            where[axis] = value
        return where

    def to_c(self, part, name, a, b):
        self.ring_start(part, name, 2, a, b)
        self.across(part, self.unit(part, a, b, 0), int(b == 2))

    def begin(self):
        self.parts = []
        for number, (low, high, first) in enumerate(PARTS):
            axes = (first, (first + 1) % 3, (first + 2) % 3)
            self.parts.append(dict(number=number, axes=axes, tiles=slice(low, high)))
        for order, name in enumerate(("A", "B0", "C0")):
            for part in self.parts:
                self.ring_start(part, name, order, 0, 0)
        for part in self.parts:
            self.across(part, [0, 0, 0], 0)

    def first_axis(self, parts):
        for part in parts:
            self.wait(self.as_many(part, ("A",), REST), self.sem(part, "A"))
            self.ring_start(part, "B1", 1, REST, 0)

    def home_blocks(self, parts):
        for name in ("B0", "C0"):
            for part in parts:
                self.near(part, (name,))
        for part in parts:
            self.to_c(part, "C1", REST, 0)

    def second_axis(self, parts):
        for part in parts:
            self.near(part, ("B1",))
        for part in parts:
            self.to_c(part, "C2", EVERY, 3)
            self.to_c(part, "C3", EVERY, 1)

    def second_axis_end(self, parts):
        for part in parts:
            self.end(part, ("B0", "B1"))
            self.to_c(part, "C4", EVERY, 2)

    def third_axis_line(self, parts):
        for part in parts:
            self.near(part, ("C1",))
            self.across(part, self.unit(part, EVERY, 0, 3), 0)
            self.across(part, self.unit(part, EVERY, 0, 1), 0)

    def third_axis(self, parts, pairs):
        for part in parts:
            self.near(part, tuple(name for name, _ in pairs))
            for _, b in pairs:
                self.across(part, self.unit(part, EVERY, b, 3), int(b == 2))
                self.across(part, self.unit(part, EVERY, b, 1), int(b == 2))

    def third_axis_line_end(self, parts):
        for part in parts:
            self.end(part, ("C0", "C1"))
            self.across(part, self.unit(part, EVERY, 0, 2), 1)

    def third_axis_end(self, parts, pairs):
        for part in parts:
            self.end(part, tuple(name for name, _ in pairs))
            for _, b in pairs:
                self.across(part, self.unit(part, EVERY, b, 2), 1 + int(b == 2))

    def wait_partner_first(self):
        low = PARTS[0][1]
        assert 28 * low == 4 * (TILES - low)
        self.wait(self.qbuf.at[:, 0, 0, 1, slice(low, TILES)], self.cross_sem.at[0])

    def wait_partner(self, wave):
        ys, zs = (slice(0, 3), slice(0, 3), slice(0, 1))[wave], (slice(0, 3), slice(0, 2), slice(0, 1))[wave]
        ref = self.qbuf.at[:, ys, zs, 1, slice(PARTS[0][1] if wave else 0, TILES)]
        self.wait(ref, self.cross_sem.at[wave + 1])

    def drain(self):
        rest = slice(1, SIDE)
        for ref in (
            self.qbuf.at[rest], self.qbuf.at[0, rest], self.qbuf.at[0, 0, rest], self.qbuf.at[0, 0, 0, 1]
        ):
            pltpu.make_async_copy(ref, ref, self.send_sem).wait()


def kernel(
    q_hbm, docs_hbm, lengths_hbm, sdev_hbm, slist_hbm, srow_hbm, pdev_hbm, plist_hbm,
    out_ref,
    lengths, sdev_ref, slist_ref, srow_ref, pdev_ref, plist_ref,
    qbuf, docs, dpre, gath, oh, sel, slot_ref, psel, ask, asked, psend, precv, rsend, rrecv,
    known, small_sem, load_sem, gsend, grecv, gcross, xsend, xrecv,
):
    me = coords()
    own_number = (me[0] * SIDE + me[1]) * 8 + me[2] * 2 + me[3]
    peers = Peers(me)
    barrier = pltpu.get_barrier_semaphore()
    gather = Gather(qbuf, gsend, grecv, gcross, me)
    lines = [[gather.peers[axis, step] for step in (2, 1, 3)] for axis in range(3)]

    def tell(sem, them):
        for peer in them:
            pl.semaphore_signal(sem, inc=1, device_id=peer, device_id_type=MESH)

    others = [(gx, gather.partner[1]) for gx, _ in lines[0]] + [gather.partner]
    tell(barrier, lines[0] + others + lines[1] + lines[2])

    for t in range(TILES):
        pltpu.make_async_copy(
            q_hbm.at[:, pl.ds(t * 128, 128)], qbuf.at[0, 0, 0, 0, t], load_sem.at[0]
        ).start()
    small = [
        pltpu.make_async_copy(src, dst, small_sem.at[n])
        for n, (src, dst) in enumerate((
            (sdev_hbm, sdev_ref), (slist_hbm, slist_ref), (srow_hbm, srow_ref),
            (pdev_hbm, pdev_ref), (plist_hbm, plist_ref), (lengths_hbm, lengths),
        ))
    ]
    for copy in small:
        copy.start()
    docs_copy = pltpu.make_async_copy(docs_hbm.at[:, pl.ds(0, ELIG), :], docs, load_sem.at[1])
    docs_copy.start()
    dpre_copy = pltpu.make_async_copy(docs_hbm.at[:, :, pl.ds(0, PREFIX)], dpre, load_sem.at[2])
    dpre_copy.start()

    pltpu.make_async_copy(qbuf.at[0, 0, 0, 1], qbuf.at[0, 0, 0, 0], load_sem.at[0]).wait()
    pl.semaphore_wait(barrier, 13)
    tell(known.at[0], lines[1])
    gather.begin()
    for copy in small:
        copy.wait()

    dev = iota((QROWS, DEVS), 1)
    sdev = sdev_ref[...]
    scode = (slist_ref[...] * ELIG + srow_ref[...] + 1).astype(F32)
    pdev = pdev_ref[...]
    pcode = (plist_ref[...] + 1).astype(F32)
    lower = (iota((QROWS, QROWS), 1) < iota((QROWS, QROWS), 0)).astype(F32).astype(BF16)
    qnum = iota((QROWS, DEVS), 0).astype(F32) + 1.0

    def table(devs, codes, width):
        got = jnp.zeros((QROWS, DEVS), F32)
        for s in range(width):
            got = got + jnp.where(devs[:, s : s + 1] == dev, codes[:, s : s + 1], 0.0)
        used = jnp.where(got > 0.0, 1.0, 0.0)
        rank = jnp.dot(lower, used.astype(BF16), preferred_element_type=F32)
        return got, jnp.where(used > 0.0, rank, -1.0)

    stab, srank = table(sdev, scode, SHORT)
    ptab, prank = table(pdev, pcode, PROBES)
    krow = iota((16, DEVS), 0)
    slots = jnp.zeros((16, DEVS), F32)
    for base, row_base, tab, rank, cap in (
        (LANE_CODE, LANE_ROW, stab, srank, CAP),
        (LANE_LIST, LANE_PROW, ptab, prank, PCAP),
    ):
        for j in range(cap):
            hit = rank == float(j)
            code = jnp.sum(jnp.where(hit, tab, 0.0), axis=0, keepdims=True) - 1.0
            row = jnp.sum(jnp.where(hit, qnum, 0.0), axis=0, keepdims=True) - 1.0
            slots = jnp.where(krow == base + j, code, slots)
            slots = jnp.where(krow == row_base + j, row, slots)
    slots = jnp.concatenate([slots, jnp.zeros((112, DEVS), F32)], axis=0).T
    ask[...] = slots.astype(I32).reshape(DEVS, 1, DEVS)

    def exchange_rows(src, dst, peer, number):
        pltpu.make_async_remote_copy(
            src_ref=src, dst_ref=dst, send_sem=xsend.at[number], recv_sem=xrecv.at[number],
            device_id=peer, device_id_type=MESH,
        ).start()

    def exchanged(send, recv, number, rows):
        some = pl.ds(0, rows)
        pltpu.make_async_copy(recv.at[some], recv.at[some], xrecv.at[number]).wait()
        pltpu.make_async_copy(send.at[some], send.at[some], xsend.at[number]).wait()

    def ask_peer(peer, flat, off, back):
        exchange_rows(ask.at[flat], asked.at[back], peer, back % CHIPS // HALF)


    lane = iota((16, DEVS), 1)

    def read_slots(half):
        exchanged(ask, asked, half, DEVS // 2 - (half == 0))
        if half == 0:
            asked[0] = ask[own_number]
        for core in range(2):
            here = pl.ds(core * CHIPS + half * HALF, HALF)
            slot_ref[here] = asked[here].reshape(HALF, DEVS)
        doc_number = iota((HALF, LISTS * ELIG), 1)
        for j in range(CAP):
            for core in range(2):
                here = pl.ds(core * CHIPS + half * HALF, HALF)
                hit = slot_ref[here, LANE_CODE + j : LANE_CODE + j + 1] == doc_number
                oh[half, pl.ds((j * 2 + core) * HALF, HALF), :] = jnp.where(hit, 1.0, 0.0).astype(BF16)

    def pick(half, low, high):
        def body(n, carry):
            cols = pl.ds(pl.multiple_of(n * 512, 512), 512)
            block = docs[:, :, cols].reshape(LISTS * ELIG, 512)
            got = jnp.dot(oh[half], block, preferred_element_type=F32)
            gath[:, :, pl.ds(half * HALF, HALF), cols] = got.astype(BF16).reshape(CAP, 2, HALF, 512)
            return carry

        lax.fori_loop(low, high, body, 0)

    group_row = iota((16, 1), 0)
    group_col = iota((16, 256), 1)

    def blocks(start, stop, low, high):
        places = [(*BLOCKS[off % CHIPS], off // CHIPS) for off in range(start, stop)]
        tiles = [
            jnp.concatenate([qbuf[y, x, z, c, t] for y, x, z, c in places], axis=0)
            for t in range(low, high)
        ]
        return jnp.concatenate(tiles, axis=1)

    def queries(g, low, high):
        return blocks(g * 16, g * 16 + 16, low, high)

    def column(g, at):
        number = slot_ref[pl.ds(g * 16, 16), at : at + 1]
        return jnp.where(number < 0, -1, group_row * QROWS + number)

    def prefix_scores():
        for g in range(2 * SIDE):
            hits = [jnp.where(column(g, LANE_PROW + p) == group_col, 1.0, 0.0) for p in range(PCAP)]
            hit = jnp.concatenate(hits, axis=0).astype(BF16)
            rows = jnp.dot(hit, queries(g, 0, PREFIX // 128), preferred_element_type=F32)
            norm = jnp.sqrt(1.0 + jnp.sum(rows * rows, axis=1, keepdims=True))
            rows = rows / norm
            for p in range(PCAP):
                psel[pl.ds(p * DEVS + g * 16, 16), :] = rows[p * 16 : (p + 1) * 16, :]
        slot_t = slot_ref[...].astype(F32).T
        lists = jnp.concatenate(
            [slot_t[LANE_LIST + p : LANE_LIST + p + 1, :] for p in range(PCAP)], axis=1
        )
        wanted = psel[...].T.astype(BF16)
        sel[...] = jnp.zeros_like(sel)
        for n in range(LISTS):
            got = jnp.dot(dpre[n], wanted, preferred_element_type=F32)
            sel[...] = jnp.where(lists == float(n), got, sel[...])
        rows_valid = jnp.zeros((1, PCAP * DEVS), I32)
        for n in range(LISTS):
            rows_valid = jnp.where(lists == float(n), lengths[n], rows_valid)
        sub = iota((8, DEVS), 0)
        tops = []
        for p in range(PCAP):
            lanes = pl.ds(p * DEVS, DEVS)
            bound = rows_valid[:, p * DEVS : (p + 1) * DEVS]
            seq = [
                jnp.where(sub + v * 8 < bound, sel[pl.ds(v * 8, 8), lanes], LOW) for v in range(32)
            ]
            seq = sort_down(seq)
            for shift in (4, 2, 1):
                seq = join_rolled(seq, shift, 0)
            for m in range(TOPK // 8):
                block = seq[m * 8]
                for s in range(1, 8):
                    block = jnp.where(sub == s, seq[m * 8 + s], block)
                tops.append(block)
        tops.append(jnp.zeros((DEVS - PCAP * TOPK, DEVS), F32))
        psend[...] = jnp.concatenate(tops, axis=0).T.reshape(DEVS, 1, DEVS)

    def return_prefix():
        peers.each(lambda peer, flat, off, back: exchange_rows(psend.at[off], precv.at[own_number], peer, 2))

    def merge_prefix():
        exchanged(psend, precv, 2, DEVS - 1)
        precv[own_number] = psend[0]
        back = precv[...].reshape(DEVS, DEVS).T
        first, second = prank == 0.0, prank == 1.0
        seq = [
            jnp.where(
                first, back[k : k + 1, :], jnp.where(second, back[TOPK + k : TOPK + k + 1, :], LOW)
            )
            for k in range(TOPK)
        ]
        for shift in (64, 32, 16, 8, 4, 2, 1):
            seq = join_rolled(seq, shift, 1)
        best = seq[0]
        for k in range(1, TOPK):
            best = jnp.where(lane == k, seq[k], best)
        out_ref[...] = best

    def rescore(wave, core):
        start, stop = WAVES[wave]
        low, high = start // 16 * 16, -(-stop // 16) * 16
        rows, cols = high - low, (stop - start) * QROWS
        left = gath[:, core, pl.ds(low, rows), :].reshape(CAP * rows, FULL)
        start, stop, low = start + core * CHIPS, stop + core * CHIPS, low + core * CHIPS
        got = lax.dot_general(
            left, blocks(start, stop, 0, TILES), (((1,), (1,)), ((), ())), preferred_element_type=F32
        )
        base = (iota((rows, 1), 0) + (low - start)) * QROWS
        col = iota((rows, cols), 1)
        total = jnp.zeros((rows, cols), F32)
        for j in range(CAP):
            number = slot_ref[pl.ds(low, rows), LANE_ROW + j : LANE_ROW + j + 1]
            hit = jnp.where(number < 0, -1, base + number) == col
            total = total + jnp.where(hit, got[j * rows : (j + 1) * rows, :], 0.0)
        value = jnp.sum(total, axis=0, keepdims=True)
        rest = WAVE_ROWS[wave] * 128 - cols
        value = jnp.concatenate([value, jnp.zeros((1, rest), F32)], axis=1)
        to = core * sum(WAVE_ROWS) + sum(WAVE_ROWS[:wave])
        for n in range(WAVE_ROWS[wave]):
            rsend[to + n] = value[:, n * 128 : (n + 1) * 128]
        for off in range(start, stop):
            if off:
                exchange_rows(rsend.at[to + (off - start) // 8], rrecv.at[own_number], peers.at(off), 3)

    first, others = gather.parts[:1], gather.parts[1:]
    pl.semaphore_wait(known.at[0], 3)
    tell(known.at[1], lines[2])
    gather.first_axis(first)
    gather.first_axis(others)
    pl.semaphore_wait(known.at[1], 3)
    peers.each(ask_peer, near_half_first=True)
    gather.home_blocks(first)
    gather.home_blocks(others)
    docs_copy.wait()
    dpre_copy.wait()
    gather.second_axis(first)
    gather.second_axis(others)
    gather.third_axis_line(first)
    gather.second_axis_end(first)
    gather.third_axis_line(others)
    read_slots(0)
    pick(0, 0, 2)
    gather.second_axis_end(others)
    gather.third_axis(first, NEAR)
    pick(0, 2, 4)
    read_slots(1)
    pick(1, 0, 2)
    gather.third_axis(others, NEAR)
    gather.third_axis(first, FAR)
    gather.third_axis_line_end(first)
    pick(1, 2, 4)
    rescore(0, 0)
    gather.third_axis_end(first, NEAR)
    gather.third_axis_end(first, FAR)
    gather.third_axis(others, FAR)
    gather.wait_partner(0)
    rescore(0, 1)
    gather.third_axis_line_end(others)
    gather.third_axis_end(others, NEAR)
    gather.wait_partner_first()
    prefix_scores()
    return_prefix()
    gather.third_axis_end(others, FAR)
    rescore(2, 0)
    rescore(1, 0)
    gather.wait_partner(1)
    gather.wait_partner(2)
    rescore(2, 1)
    rescore(1, 1)
    gather.drain()
    merge_prefix()
    squares = jnp.zeros((QROWS, 128), F32)
    for t in range(TILES):
        value = qbuf[0, 0, 0, 0, t].astype(F32)
        squares = squares + value * value
    full_norm = jnp.sqrt(1.0 + jnp.sum(squares, axis=1, keepdims=True))
    other = iota((16, DEVS), 1)
    seen = (me[0] + SIDE - other // 32) % SIDE * 16 + (me[1] + SIDE - other // 8 % SIDE) % SIDE * 4
    seen = seen + (me[2] + SIDE - other // 2 % SIDE) % SIDE
    place = jnp.zeros((QROWS, DEVS), I32)
    for low, high in WAVES:
        for n in range(low, high):
            y, x, z = BLOCKS[n]
            place = jnp.where(seen == y * 16 + x * 4 + z, (n - low) % 8, place)
    exchanged(rrecv, rrecv, 3, DEVS - 1)
    rrecv[own_number] = rsend[0]
    back = rrecv[...].reshape(DEVS, DEVS).T
    value = jnp.zeros((QROWS, DEVS), F32)
    for n in range(8):
        value = jnp.where(place == n, back[n * 16 : (n + 1) * 16, :], value)
    out = jnp.zeros((QROWS, DEVS), F32)
    for s in range(SHORT):
        one = jnp.sum(jnp.where(sdev[:, s : s + 1] == dev, value, 0.0), axis=1, keepdims=True)
        out = jnp.where(lane == s, one, out)
    out_ref[:, pl.ds(TOPK, SHORT)] = (out / full_norm)[:, :SHORT]


def shards(queries, probe_dev, probe_list, documents, lengths, short_dev, short_list, short_row):
    vmem = pl.BlockSpec(memory_space=pltpu.VMEM)
    anywhere = pl.BlockSpec(memory_space=pl.ANY)
    out = pl.pallas_call(
        kernel,
        name="search",
        out_shape=pltpu.VMEM((QROWS, DEVS), F32),
        in_specs=[anywhere] * 8,
        out_specs=vmem,
        scratch_shapes=[
            pltpu.SMEM((LISTS,), I32),
            pltpu.VMEM((QROWS, SHORT), I32),
            pltpu.VMEM((QROWS, SHORT), I32),
            pltpu.VMEM((QROWS, SHORT), I32),
            pltpu.VMEM((QROWS, PROBES), I32),
            pltpu.VMEM((QROWS, PROBES), I32),
            pltpu.VMEM((SIDE, SIDE, SIDE, 2, TILES, QROWS, 128), BF16),
            pltpu.VMEM((LISTS, ELIG, FULL), BF16),
            pltpu.VMEM((LISTS, ROWS, PREFIX), BF16),
            pltpu.VMEM((CAP, 2, CHIPS, FULL), BF16),
            pltpu.VMEM((2, CAP * CHIPS, LISTS * ELIG), BF16),
            pltpu.VMEM((ROWS, PCAP * DEVS), F32),
            pltpu.VMEM((DEVS, DEVS), I32),
            pltpu.VMEM((PCAP * DEVS, PREFIX), F32),
            pltpu.VMEM((DEVS, 1, DEVS), I32),
            pltpu.VMEM((DEVS, 1, DEVS), I32),
            pltpu.VMEM((DEVS, 1, DEVS), F32),
            pltpu.VMEM((DEVS, 1, DEVS), F32),
            pltpu.VMEM((2 * sum(WAVE_ROWS), 1, DEVS), F32),
            pltpu.VMEM((DEVS, 1, DEVS), F32),
            pltpu.SemaphoreType.REGULAR((2,)),
            pltpu.SemaphoreType.DMA((6,)),
            pltpu.SemaphoreType.DMA((3,)),
            pltpu.SemaphoreType.DMA,
            pltpu.SemaphoreType.DMA((11 * len(PARTS),)),
            pltpu.SemaphoreType.DMA((4,)),
            pltpu.SemaphoreType.DMA((4,)),
            pltpu.SemaphoreType.DMA((4,)),
        ],
        compiler_params=pltpu.CompilerParams(
            collective_id=0, has_side_effects=True, vmem_limit_bytes=60 * 1024 * 1024
        ),
    )(queries, documents, lengths, short_dev, short_list, short_row, probe_dev, probe_list)
    return out[:, :TOPK], out[:, TOPK : TOPK + SHORT]


def solution(mesh):
    spread = P(("gx", "gy"), None)
    in_specs = (spread, spread, spread, P(("gx", "gy"), None, None), P(("gx", "gy")), spread, spread, spread)
    return jax.shard_map(shards, mesh=mesh, in_specs=in_specs, out_specs=(spread, spread), check_vma=False)
```

```python
import jax
import jax.numpy as jnp
from jax import lax
from jax.experimental import pallas as pl
from jax.experimental.pallas import tpu as pltpu
from jax.sharding import PartitionSpec as P

MESH = pl.DeviceIdType.MESH
SIDE = 4
DEVS = 128
QROWS = 16
LISTS = 16
ROWS = 256
ELIG = 96
PREFIX = 256
FULL = 2048
TILES = FULL // 128
CAP = 5
PCAP = 2
TOPK = 32
SHORT = 32
PROBES = 16
LOW = -1e30
PARTS = ((0, 2, 2), (2, 7, 0), (7, 12, 1), (12, 16, 2))
F32 = jnp.float32
BF16 = jnp.bfloat16
I32 = jnp.int32
LANE_CODE, LANE_ROW, LANE_LIST, LANE_PROW = 0, 5, 10, 12


def iota(shape, axis):
    return lax.broadcasted_iota(I32, shape, axis)


def merge_down(seq):
    seq = list(seq)
    step = len(seq) // 2
    while step:
        for i in range(len(seq)):
            if not i & step:
                a, b = seq[i], seq[i + step]
                seq[i], seq[i + step] = jnp.maximum(a, b), jnp.minimum(a, b)
        step //= 2
    return seq


def sort_down(seq):
    if len(seq) == 1:
        return list(seq)
    half = len(seq) // 2
    return merge_down(sort_down(seq[:half]) + sort_down(seq[half:])[::-1])


def join_rolled(seq, shift, axis):
    count = len(seq)
    other = [pltpu.roll(v, shift, axis) for v in seq]
    return merge_down([jnp.maximum(seq[i], other[count - 1 - i]) for i in range(count)])


def coords():
    gx, gy = lax.axis_index("gx"), lax.axis_index("gy")
    return gx // SIDE, gx % SIDE, gy // 2, gy % 2


def device_of(y, x, z, c):
    return (y * SIDE + x, z * 2 + c)


FAR_FIRST = (2, 1, 3, 0)
BLOCKS = sorted(
    ((y, x, z) for y in range(SIDE) for x in range(SIDE) for z in range(SIDE)),
    key=lambda b: (min(2, sum(v == 2 for v in b)), b),
)
CHIPS = len(BLOCKS)
HALF = CHIPS // 2
WAVES = ((0, 27), (27, 54), (54, 64))
WAVE_ROWS = (4, 4, 2)
EVERY, REST = slice(0, SIDE), slice(1, SIDE)
NEAR, FAR = (("C2", 3), ("C3", 1)), (("C4", 2),)
NEAR_SEM = dict(A="A", B0="B0", C0="C0", B1="B1", C1="C1", C2="C23", C3="C23", C4="C4")
END_SEM = dict(A="A", B0="B_", B1="B_", C0="C01_", C1="C01_", C2="C23_", C3="C23_", C4="C4_")
STRAIGHT_FIRST, STRAIGHT = ("A", "B0", "B1", "C4"), ("A",)


class Peers:
    def __init__(self, me):
        rows = [(me[0] + d) % SIDE * SIDE for d in range(SIDE)]
        xs = [(me[1] + d) % SIDE for d in range(SIDE)]
        zs = [(me[2] + d) % SIDE * 2 for d in range(SIDE)]
        self.gxs = [[row + x for x in xs] for row in rows]
        self.gys = [[z + me[3], z + 1 - me[3]] for z in zs]

    def at(self, off):
        y, x, z = BLOCKS[off % CHIPS]
        return self.gxs[y][x], self.gys[z][off // CHIPS]

    def each(self, visit, near_half_first=False):
        def order(off):
            return near_half_first and off % CHIPS // HALF, -sum(min(v, SIDE - v) for v in BLOCKS[off % CHIPS])

        for off in sorted(range(1, DEVS), key=order):
            gx, gy = self.at(off)
            back = tuple((SIDE - v) % SIDE for v in BLOCKS[off % CHIPS])
            visit((gx, gy), gx * 8 + gy, off, off // CHIPS * CHIPS + BLOCKS.index(back))


class Gather:
    def __init__(self, qbuf, send_sem, recv_sem, cross_sem, me):
        self.qbuf, self.send_sem, self.recv_sem = qbuf, send_sem, recv_sem
        self.cross_sem, self.me = cross_sem, me
        self.sems = {}
        y, x, z, c = me
        self.partner = device_of(y, x, z, 1 - c)
        self.peers = {}
        for axis in range(3):
            for step in (1, 2, 3):
                place = list(me)
                place[axis] = (place[axis] + step) % SIDE
                self.peers[axis, step] = device_of(*place)

    def view(self, where, tiles, core=0):
        return self.qbuf.at[where[0], where[1], where[2], core, tiles]

    def start(self, src, dst, peer, sem):
        pltpu.make_async_remote_copy(
            src_ref=src, dst_ref=dst, send_sem=self.send_sem, recv_sem=sem,
            device_id=peer, device_id_type=MESH,
        ).start()

    def sem(self, part, name):
        key = part["number"], name
        if key not in self.sems:
            self.sems[key] = len(self.sems)
        return self.recv_sem.at[self.sems[key]]

    def slot(self, part, name, value, tiles=None):
        unit, axis = part[name]
        where = list(unit)
        where[axis] = value
        return self.view(where, tiles or part["tiles"])

    def ring_start(self, part, name, order, a, b):
        axis = part["axes"][order]
        part[name] = self.unit(part, a, b, 0), axis
        own = self.slot(part, name, 0)
        near = self.sem(part, NEAR_SEM[name])
        self.start(own, self.slot(part, name, 3), self.peers[axis, 1], near)
        self.start(own, self.slot(part, name, 1), self.peers[axis, 3], near)
        if self.straight(part, name):
            self.start(own, self.slot(part, name, 2), self.peers[axis, 2], self.sem(part, END_SEM[name]))

    def straight(self, part, name):
        return name in (STRAIGHT_FIRST if part["number"] == 0 else STRAIGHT)

    def wait(self, ref, sem):
        pltpu.make_async_copy(ref, ref, sem).wait()

    def near(self, part, names):
        self.wait(self.as_many(part, names, slice(1, 3)), self.sem(part, NEAR_SEM[names[0]]))
        tiles = part["tiles"]
        middle = (tiles.start + tiles.stop) // 2
        for name in names:
            if self.straight(part, name):
                continue
            end = self.sem(part, END_SEM[name])
            axis = part[name][1]
            for value, step, piece in ((3, 1, slice(tiles.start, middle)), (1, 3, slice(middle, tiles.stop))):
                self.start(
                    self.slot(part, name, value, piece), self.slot(part, name, 2, piece), self.peers[axis, step], end
                )

    def end(self, part, names):
        self.wait(self.as_many(part, names, 2), self.sem(part, END_SEM[names[0]]))

    def as_many(self, part, names, value):
        unit, axis = part[names[0]]
        where = list(unit)
        where[axis] = value
        if names in (("B0", "B1"), ("C0", "C1")):
            where[part["axes"][0]] = EVERY
        elif len(names) > 1:
            where[part["axes"][1]] = slice(0, len(names))
        return self.view(where, part["tiles"])

    def across(self, part, where, wave):
        tiles = part["tiles"]
        sem = self.cross_sem.at[wave + 1 if part["number"] or wave == 0 else 0]
        self.start(self.view(where, tiles, 0), self.view(where, tiles, 1), self.partner, sem)

    def unit(self, part, a, b, c):
        where = [0, 0, 0]
        for axis, value in zip(part["axes"], (a, b, c)):
            where[axis] = value
        return where

    def to_c(self, part, name, a, b):
        self.ring_start(part, name, 2, a, b)
        self.across(part, self.unit(part, a, b, 0), int(b == 2))

    def begin(self):
        self.parts = []
        for number, (low, high, first) in enumerate(PARTS):
            axes = (first, (first + 1) % 3, (first + 2) % 3)
            self.parts.append(dict(number=number, axes=axes, tiles=slice(low, high)))
        for order, name in enumerate(("A", "B0", "C0")):
            for part in self.parts:
                self.ring_start(part, name, order, 0, 0)
        for part in self.parts:
            self.across(part, [0, 0, 0], 0)

    def first_axis(self, parts):
        for part in parts:
            self.wait(self.as_many(part, ("A",), REST), self.sem(part, "A"))
            self.ring_start(part, "B1", 1, REST, 0)

    def home_blocks(self, parts):
        for name in ("B0", "C0"):
            for part in parts:
                self.near(part, (name,))
        for part in parts:
            self.to_c(part, "C1", REST, 0)

    def second_axis(self, parts):
        for part in parts:
            self.near(part, ("B1",))
        for part in parts:
            self.to_c(part, "C2", EVERY, 3)
            self.to_c(part, "C3", EVERY, 1)

    def second_axis_end(self, parts):
        for part in parts:
            self.end(part, ("B0", "B1"))
            self.to_c(part, "C4", EVERY, 2)

    def third_axis_line(self, parts):
        for part in parts:
            self.near(part, ("C1",))
            self.across(part, self.unit(part, EVERY, 0, 3), 0)
            self.across(part, self.unit(part, EVERY, 0, 1), 0)

    def third_axis(self, parts, pairs):
        for part in parts:
            self.near(part, tuple(name for name, _ in pairs))
            for _, b in pairs:
                self.across(part, self.unit(part, EVERY, b, 3), int(b == 2))
                self.across(part, self.unit(part, EVERY, b, 1), int(b == 2))

    def third_axis_line_end(self, parts):
        for part in parts:
            self.end(part, ("C0", "C1"))
            self.across(part, self.unit(part, EVERY, 0, 2), 1)

    def third_axis_end(self, parts, pairs):
        for part in parts:
            self.end(part, tuple(name for name, _ in pairs))
            for _, b in pairs:
                self.across(part, self.unit(part, EVERY, b, 2), 1 + int(b == 2))

    def wait_partner_first(self):
        low = PARTS[0][1]
        assert 28 * low == 4 * (TILES - low)
        self.wait(self.qbuf.at[:, 0, 0, 1, slice(low, TILES)], self.cross_sem.at[0])

    def wait_partner(self, wave):
        ys, zs = (slice(0, 3), slice(0, 3), slice(0, 1))[wave], (slice(0, 3), slice(0, 2), slice(0, 1))[wave]
        ref = self.qbuf.at[:, ys, zs, 1, slice(PARTS[0][1] if wave else 0, TILES)]
        self.wait(ref, self.cross_sem.at[wave + 1])

    def drain(self):
        rest = slice(1, SIDE)
        for ref in (
            self.qbuf.at[rest], self.qbuf.at[0, rest], self.qbuf.at[0, 0, rest], self.qbuf.at[0, 0, 0, 1]
        ):
            pltpu.make_async_copy(ref, ref, self.send_sem).wait()


def kernel(
    q_hbm, docs_hbm, lengths_hbm, sdev_hbm, slist_hbm, srow_hbm, pdev_hbm, plist_hbm,
    out_ref,
    lengths, sdev_ref, slist_ref, srow_ref, pdev_ref, plist_ref,
    qbuf, docs, dpre, gath, oh, sel, slot_ref, psel, ask, asked, psend, precv, rsend, rrecv,
    known, small_sem, load_sem, gsend, grecv, gcross, xsend, xrecv,
):
    me = coords()
    own_number = (me[0] * SIDE + me[1]) * 8 + me[2] * 2 + me[3]
    peers = Peers(me)
    barrier = pltpu.get_barrier_semaphore()
    gather = Gather(qbuf, gsend, grecv, gcross, me)
    lines = [[gather.peers[axis, step] for step in (2, 1, 3)] for axis in range(3)]

    def tell(sem, them):
        for peer in them:
            pl.semaphore_signal(sem, inc=1, device_id=peer, device_id_type=MESH)

    others = [(gx, gather.partner[1]) for gx, _ in lines[0]] + [gather.partner]
    tell(barrier, lines[0] + others + lines[1] + lines[2])

    for t in range(TILES):
        pltpu.make_async_copy(
            q_hbm.at[:, pl.ds(t * 128, 128)], qbuf.at[0, 0, 0, 0, t], load_sem.at[0]
        ).start()
    small = [
        pltpu.make_async_copy(src, dst, small_sem.at[n])
        for n, (src, dst) in enumerate((
            (sdev_hbm, sdev_ref), (slist_hbm, slist_ref), (srow_hbm, srow_ref),
            (pdev_hbm, pdev_ref), (plist_hbm, plist_ref), (lengths_hbm, lengths),
        ))
    ]
    for copy in small:
        copy.start()
    docs_copy = pltpu.make_async_copy(docs_hbm.at[:, pl.ds(0, ELIG), :], docs, load_sem.at[1])
    docs_copy.start()
    dpre_copy = pltpu.make_async_copy(docs_hbm.at[:, :, pl.ds(0, PREFIX)], dpre, load_sem.at[2])
    dpre_copy.start()

    pltpu.make_async_copy(qbuf.at[0, 0, 0, 1], qbuf.at[0, 0, 0, 0], load_sem.at[0]).wait()
    pl.semaphore_wait(barrier, 13)
    tell(known.at[0], lines[1])
    gather.begin()
    for copy in small:
        copy.wait()

    dev = iota((QROWS, DEVS), 1)
    sdev = sdev_ref[...]
    scode = (slist_ref[...] * ELIG + srow_ref[...] + 1).astype(F32)
    pdev = pdev_ref[...]
    pcode = (plist_ref[...] + 1).astype(F32)
    lower = (iota((QROWS, QROWS), 1) < iota((QROWS, QROWS), 0)).astype(F32).astype(BF16)
    qnum = iota((QROWS, DEVS), 0).astype(F32) + 1.0

    def table(devs, codes, width):
        got = jnp.zeros((QROWS, DEVS), F32)
        for s in range(width):
            got = got + jnp.where(devs[:, s : s + 1] == dev, codes[:, s : s + 1], 0.0)
        used = jnp.where(got > 0.0, 1.0, 0.0)
        rank = jnp.dot(lower, used.astype(BF16), preferred_element_type=F32)
        return got, jnp.where(used > 0.0, rank, -1.0)

    stab, srank = table(sdev, scode, SHORT)
    ptab, prank = table(pdev, pcode, PROBES)
    krow = iota((16, DEVS), 0)
    slots = jnp.zeros((16, DEVS), F32)
    for base, row_base, tab, rank, cap in (
        (LANE_CODE, LANE_ROW, stab, srank, CAP),
        (LANE_LIST, LANE_PROW, ptab, prank, PCAP),
    ):
        for j in range(cap):
            hit = rank == float(j)
            code = jnp.sum(jnp.where(hit, tab, 0.0), axis=0, keepdims=True) - 1.0
            row = jnp.sum(jnp.where(hit, qnum, 0.0), axis=0, keepdims=True) - 1.0
            slots = jnp.where(krow == base + j, code, slots)
            slots = jnp.where(krow == row_base + j, row, slots)
    slots = jnp.concatenate([slots, jnp.zeros((112, DEVS), F32)], axis=0).T
    ask[...] = slots.astype(I32).reshape(DEVS, 1, DEVS)

    def exchange_rows(src, dst, peer, number):
        pltpu.make_async_remote_copy(
            src_ref=src, dst_ref=dst, send_sem=xsend.at[number], recv_sem=xrecv.at[number],
            device_id=peer, device_id_type=MESH,
        ).start()

    def exchanged(send, recv, number, rows):
        some = pl.ds(0, rows)
        pltpu.make_async_copy(recv.at[some], recv.at[some], xrecv.at[number]).wait()
        pltpu.make_async_copy(send.at[some], send.at[some], xsend.at[number]).wait()

    def ask_peer(peer, flat, off, back):
        exchange_rows(ask.at[flat], asked.at[back], peer, back % CHIPS // HALF)


    lane = iota((16, DEVS), 1)

    def read_slots(half):
        exchanged(ask, asked, half, DEVS // 2 - (half == 0))
        if half == 0:
            asked[0] = ask[own_number]
        for core in range(2):
            here = pl.ds(core * CHIPS + half * HALF, HALF)
            slot_ref[here] = asked[here].reshape(HALF, DEVS)
        doc_number = iota((HALF, LISTS * ELIG), 1)
        for j in range(CAP):
            for core in range(2):
                here = pl.ds(core * CHIPS + half * HALF, HALF)
                hit = slot_ref[here, LANE_CODE + j : LANE_CODE + j + 1] == doc_number
                oh[half, pl.ds((j * 2 + core) * HALF, HALF), :] = jnp.where(hit, 1.0, 0.0).astype(BF16)

    def pick(half, low, high):
        def body(n, carry):
            cols = pl.ds(pl.multiple_of(n * 1024, 1024), 1024)
            block = docs[:, :, cols].reshape(LISTS * ELIG, 1024)
            got = jnp.dot(oh[half], block, preferred_element_type=F32)
            gath[:, :, pl.ds(half * HALF, HALF), cols] = got.astype(BF16).reshape(CAP, 2, HALF, 1024)
            return carry

        lax.fori_loop(low, high, body, 0)

    group_row = iota((16, 1), 0)
    group_col = iota((16, 256), 1)

    def blocks(start, stop, low, high):
        places = [(*BLOCKS[off % CHIPS], off // CHIPS) for off in range(start, stop)]
        tiles = [
            jnp.concatenate([qbuf[y, x, z, c, t] for y, x, z, c in places], axis=0)
            for t in range(low, high)
        ]
        return jnp.concatenate(tiles, axis=1)

    def queries(g, low, high):
        return blocks(g * 16, g * 16 + 16, low, high)

    def column(g, at):
        number = slot_ref[pl.ds(g * 16, 16), at : at + 1]
        return jnp.where(number < 0, -1, group_row * QROWS + number)

    def prefix_scores():
        for g in range(2 * SIDE):
            hits = [jnp.where(column(g, LANE_PROW + p) == group_col, 1.0, 0.0) for p in range(PCAP)]
            hit = jnp.concatenate(hits, axis=0).astype(BF16)
            rows = jnp.dot(hit, queries(g, 0, PREFIX // 128), preferred_element_type=F32)
            norm = jnp.sqrt(1.0 + jnp.sum(rows * rows, axis=1, keepdims=True))
            rows = rows / norm
            for p in range(PCAP):
                psel[pl.ds(p * DEVS + g * 16, 16), :] = rows[p * 16 : (p + 1) * 16, :]
        slot_t = slot_ref[...].astype(F32).T
        lists = jnp.concatenate(
            [slot_t[LANE_LIST + p : LANE_LIST + p + 1, :] for p in range(PCAP)], axis=1
        )
        wanted = psel[...].T.astype(BF16)
        sel[...] = jnp.zeros_like(sel)
        for n in range(LISTS):
            got = jnp.dot(dpre[n], wanted, preferred_element_type=F32)
            sel[...] = jnp.where(lists == float(n), got, sel[...])
        rows_valid = jnp.zeros((1, PCAP * DEVS), I32)
        for n in range(LISTS):
            rows_valid = jnp.where(lists == float(n), lengths[n], rows_valid)
        sub = iota((8, DEVS), 0)
        tops = []
        for p in range(PCAP):
            lanes = pl.ds(p * DEVS, DEVS)
            bound = rows_valid[:, p * DEVS : (p + 1) * DEVS]
            seq = [
                jnp.where(sub + v * 8 < bound, sel[pl.ds(v * 8, 8), lanes], LOW) for v in range(32)
            ]
            seq = sort_down(seq)
            for shift in (4, 2, 1):
                seq = join_rolled(seq, shift, 0)
            for m in range(TOPK // 8):
                block = seq[m * 8]
                for s in range(1, 8):
                    block = jnp.where(sub == s, seq[m * 8 + s], block)
                tops.append(block)
        tops.append(jnp.zeros((DEVS - PCAP * TOPK, DEVS), F32))
        psend[...] = jnp.concatenate(tops, axis=0).T.reshape(DEVS, 1, DEVS)

    def return_prefix():
        peers.each(lambda peer, flat, off, back: exchange_rows(psend.at[off], precv.at[own_number], peer, 2))

    def merge_prefix():
        exchanged(psend, precv, 2, DEVS - 1)
        precv[own_number] = psend[0]
        back = precv[...].reshape(DEVS, DEVS).T
        first, second = prank == 0.0, prank == 1.0
        seq = [
            jnp.where(
                first, back[k : k + 1, :], jnp.where(second, back[TOPK + k : TOPK + k + 1, :], LOW)
            )
            for k in range(TOPK)
        ]
        for shift in (64, 32, 16, 8, 4, 2, 1):
            seq = join_rolled(seq, shift, 1)
        best = seq[0]
        for k in range(1, TOPK):
            best = jnp.where(lane == k, seq[k], best)
        out_ref[...] = best

    def rescore(wave, core):
        start, stop = WAVES[wave]
        low, high = start // 16 * 16, -(-stop // 16) * 16
        rows, cols = high - low, (stop - start) * QROWS
        left = gath[:, core, pl.ds(low, rows), :].reshape(CAP * rows, FULL)
        start, stop, low = start + core * CHIPS, stop + core * CHIPS, low + core * CHIPS
        got = lax.dot_general(
            left, blocks(start, stop, 0, TILES), (((1,), (1,)), ((), ())), preferred_element_type=F32
        )
        base = (iota((rows, 1), 0) + (low - start)) * QROWS
        col = iota((rows, cols), 1)
        total = jnp.zeros((rows, cols), F32)
        for j in range(CAP):
            number = slot_ref[pl.ds(low, rows), LANE_ROW + j : LANE_ROW + j + 1]
            hit = jnp.where(number < 0, -1, base + number) == col
            total = total + jnp.where(hit, got[j * rows : (j + 1) * rows, :], 0.0)
        value = jnp.sum(total, axis=0, keepdims=True)
        rest = WAVE_ROWS[wave] * 128 - cols
        value = jnp.concatenate([value, jnp.zeros((1, rest), F32)], axis=1)
        to = core * sum(WAVE_ROWS) + sum(WAVE_ROWS[:wave])
        for n in range(WAVE_ROWS[wave]):
            rsend[to + n] = value[:, n * 128 : (n + 1) * 128]
        for off in range(start, stop):
            if off:
                exchange_rows(rsend.at[to + (off - start) // 8], rrecv.at[own_number], peers.at(off), 3)

    first, others = gather.parts[:1], gather.parts[1:]
    pl.semaphore_wait(known.at[0], 3)
    tell(known.at[1], lines[2])
    gather.first_axis(first)
    gather.first_axis(others)
    pl.semaphore_wait(known.at[1], 3)
    peers.each(ask_peer, near_half_first=True)
    gather.home_blocks(first)
    gather.home_blocks(others)
    docs_copy.wait()
    dpre_copy.wait()
    gather.second_axis(first)
    gather.second_axis(others)
    gather.third_axis_line(first)
    gather.second_axis_end(first)
    gather.third_axis_line(others)
    read_slots(0)
    pick(0, 0, 1)
    gather.second_axis_end(others)
    gather.third_axis(first, NEAR)
    pick(0, 1, 2)
    read_slots(1)
    pick(1, 0, 1)
    gather.third_axis(others, NEAR)
    gather.third_axis(first, FAR)
    gather.third_axis_line_end(first)
    pick(1, 1, 2)
    rescore(0, 0)
    gather.third_axis_end(first, NEAR)
    gather.third_axis_end(first, FAR)
    gather.third_axis(others, FAR)
    gather.wait_partner(0)
    rescore(0, 1)
    gather.third_axis_line_end(others)
    gather.third_axis_end(others, NEAR)
    rescore(1, 0)
    gather.wait_partner_first()
    prefix_scores()
    gather.third_axis_end(others, FAR)
    return_prefix()
    rescore(2, 0)
    gather.wait_partner(1)
    gather.wait_partner(2)
    rescore(2, 1)
    rescore(1, 1)
    gather.drain()
    merge_prefix()
    squares = jnp.zeros((QROWS, 128), F32)
    for t in range(TILES):
        value = qbuf[0, 0, 0, 0, t].astype(F32)
        squares = squares + value * value
    full_norm = jnp.sqrt(1.0 + jnp.sum(squares, axis=1, keepdims=True))
    other = iota((16, DEVS), 1)
    seen = (me[0] + SIDE - other // 32) % SIDE * 16 + (me[1] + SIDE - other // 8 % SIDE) % SIDE * 4
    seen = seen + (me[2] + SIDE - other // 2 % SIDE) % SIDE
    place = jnp.zeros((QROWS, DEVS), I32)
    for low, high in WAVES:
        for n in range(low, high):
            y, x, z = BLOCKS[n]
            place = jnp.where(seen == y * 16 + x * 4 + z, (n - low) % 8, place)
    exchanged(rrecv, rrecv, 3, DEVS - 1)
    rrecv[own_number] = rsend[0]
    back = rrecv[...].reshape(DEVS, DEVS).T
    value = jnp.zeros((QROWS, DEVS), F32)
    for n in range(8):
        value = jnp.where(place == n, back[n * 16 : (n + 1) * 16, :], value)
    out = jnp.zeros((QROWS, DEVS), F32)
    for s in range(SHORT):
        one = jnp.sum(jnp.where(sdev[:, s : s + 1] == dev, value, 0.0), axis=1, keepdims=True)
        out = jnp.where(lane == s, one, out)
    out_ref[:, pl.ds(TOPK, SHORT)] = (out / full_norm)[:, :SHORT]


def shards(queries, probe_dev, probe_list, documents, lengths, short_dev, short_list, short_row):
    vmem = pl.BlockSpec(memory_space=pltpu.VMEM)
    anywhere = pl.BlockSpec(memory_space=pl.ANY)
    out = pl.pallas_call(
        kernel,
        name="search",
        out_shape=pltpu.VMEM((QROWS, DEVS), F32),
        in_specs=[anywhere] * 8,
        out_specs=vmem,
        scratch_shapes=[
            pltpu.SMEM((LISTS,), I32),
            pltpu.VMEM((QROWS, SHORT), I32),
            pltpu.VMEM((QROWS, SHORT), I32),
            pltpu.VMEM((QROWS, SHORT), I32),
            pltpu.VMEM((QROWS, PROBES), I32),
            pltpu.VMEM((QROWS, PROBES), I32),
            pltpu.VMEM((SIDE, SIDE, SIDE, 2, TILES, QROWS, 128), BF16),
            pltpu.VMEM((LISTS, ELIG, FULL), BF16),
            pltpu.VMEM((LISTS, ROWS, PREFIX), BF16),
            pltpu.VMEM((CAP, 2, CHIPS, FULL), BF16),
            pltpu.VMEM((2, CAP * CHIPS, LISTS * ELIG), BF16),
            pltpu.VMEM((ROWS, PCAP * DEVS), F32),
            pltpu.VMEM((DEVS, DEVS), I32),
            pltpu.VMEM((PCAP * DEVS, PREFIX), F32),
            pltpu.VMEM((DEVS, 1, DEVS), I32),
            pltpu.VMEM((DEVS, 1, DEVS), I32),
            pltpu.VMEM((DEVS, 1, DEVS), F32),
            pltpu.VMEM((DEVS, 1, DEVS), F32),
            pltpu.VMEM((2 * sum(WAVE_ROWS), 1, DEVS), F32),
            pltpu.VMEM((DEVS, 1, DEVS), F32),
            pltpu.SemaphoreType.REGULAR((2,)),
            pltpu.SemaphoreType.DMA((6,)),
            pltpu.SemaphoreType.DMA((3,)),
            pltpu.SemaphoreType.DMA,
            pltpu.SemaphoreType.DMA((11 * len(PARTS),)),
            pltpu.SemaphoreType.DMA((4,)),
            pltpu.SemaphoreType.DMA((4,)),
            pltpu.SemaphoreType.DMA((4,)),
        ],
        compiler_params=pltpu.CompilerParams(
            collective_id=0, has_side_effects=True, vmem_limit_bytes=60 * 1024 * 1024
        ),
    )(queries, documents, lengths, short_dev, short_list, short_row, probe_dev, probe_list)
    return out[:, :TOPK], out[:, TOPK : TOPK + SHORT]


def solution(mesh):
    spread = P(("gx", "gy"), None)
    in_specs = (spread, spread, spread, P(("gx", "gy"), None, None), P(("gx", "gy")), spread, spread, spread)
    return jax.shard_map(shards, mesh=mesh, in_specs=in_specs, out_specs=(spread, spread), check_vma=False)
```
